8 devices in a mesh: rep: 1 (over z), data: 2 (over y), expert: 4 (over x, core).
Axes of the slice: x: 2, y: 2, z: 1, core: 2. Of those that a mesh axis runs over, the one named last changes fastest.
Arguments:
- x: bfloat16 [32768, 2048], P(('rep', 'expert', 'data'))
- expert_idx: int32 [32768, 2], P(('rep', 'expert', 'data'))
- gate: float32 [32768, 2], P(('rep', 'expert', 'data'))
- w_gate: bfloat16 [8, 2048, 5632], P('expert', 'data')
- w_up: bfloat16 [8, 2048, 5632], P('expert', 'data')
- w_down: bfloat16 [8, 5632, 2048], P('expert', None, 'data')
Outputs:
- output: bfloat16 [32768, 2048], P(('rep', 'expert', 'data'))
All inputs are finite; a program needn't handle non-finite values.
Results may differ from the reference program's by a relative error of at most 0.001.
Values are sent between devices in bfloat16 or wider.
A program may use at most 1 GiB of HBM per device.

```python
import jax
import jax.numpy as jnp
from jax import lax

TOK_DEV = 4096
D_MODEL = 2048
FFN = 5632
EXPERTS = 8
TOP_K = 2
EP_SIZE = 4
DP_SIZE = 2
CAPACITY = 1280


def route_ids(key):
    n_blocks = EP_SIZE * DP_SIZE
    key_bias, key_hot, key_score = jax.random.split(key, 3)
    expert_bias = jax.random.randint(key_bias, (EXPERTS,), 0, 2 ** 20, dtype=jnp.int32)
    hot_expert = jax.random.randint(key_hot, (), 0, EXPERTS, dtype=jnp.int32)
    scores = jax.random.randint(key_score, (n_blocks, TOK_DEV, EXPERTS), 0, 2 ** 20, dtype=jnp.int32) + expert_bias
    forced = (jnp.arange(TOK_DEV) < CAPACITY)[None, :, None] & (jnp.arange(EXPERTS) == hot_expert)[None, None, :]
    scores = (scores + forced.astype(jnp.int32) * 2 ** 21) * EXPERTS + jnp.arange(EXPERTS, dtype=jnp.int32)
    chosen = lax.top_k(scores, TOP_K)[1]
    return chosen.reshape(n_blocks * TOK_DEV, TOP_K).astype(jnp.int32)


def setup_inputs(seed: int = 0, part: int = 0) -> dict:
    key_shared, key_local = jax.random.split(jax.random.key(seed))
    key_tok, key_route, key_gate = jax.random.split(jax.random.fold_in(key_local, part), 3)
    key_wg, key_wu, key_wd = jax.random.split(key_shared, 3)
    n_rows = EP_SIZE * DP_SIZE * TOK_DEV
    x = jax.random.normal(key_tok, (n_rows, D_MODEL), jnp.float32).astype(jnp.bfloat16)
    gate = jax.random.uniform(key_gate, (n_rows, TOP_K), jnp.float32, 0.2, 0.8)
    w_gate = (jax.random.normal(key_wg, (EXPERTS, D_MODEL, FFN), jnp.float32) * D_MODEL ** -0.5).astype(jnp.bfloat16)
    w_up = (jax.random.normal(key_wu, (EXPERTS, D_MODEL, FFN), jnp.float32) * D_MODEL ** -0.5).astype(jnp.bfloat16)
    w_down = (jax.random.normal(key_wd, (EXPERTS, FFN, D_MODEL), jnp.float32) * (1.5 * FFN ** -0.5)).astype(jnp.bfloat16)
    return {"x": x, "expert_idx": route_ids(key_route), "gate": gate, "w_gate": w_gate, "w_up": w_up, "w_down": w_down}


def slot_table(ids_flat):
    one_hot = (ids_flat[:, None] == jnp.arange(EXPERTS, dtype=jnp.int32)[None, :]).astype(jnp.int32)
    slot_ids = jnp.sum((jnp.cumsum(one_hot, axis=0) - one_hot) * one_hot, axis=1)
    return jnp.where(slot_ids < CAPACITY, ids_flat * CAPACITY + slot_ids, EXPERTS * CAPACITY)


def take_rows(block, index):
    return jnp.take(block, index, axis=0, mode="fill", fill_value=0)


def reference(x, expert_idx, gate, w_gate, w_up, w_down):
    n_blocks = EP_SIZE * DP_SIZE
    x_blocks = x.reshape(n_blocks, TOK_DEV, D_MODEL)
    dest_row = jax.vmap(slot_table)(expert_idx.reshape(n_blocks, TOK_DEV * TOP_K))
    block_ids = jnp.arange(n_blocks)[:, None]
    pair_token = jnp.broadcast_to(jnp.arange(TOK_DEV * TOP_K, dtype=jnp.int32) // TOP_K, dest_row.shape)
    src_tok = jnp.full((n_blocks, EXPERTS * CAPACITY), TOK_DEV, jnp.int32).at[block_ids, dest_row].set(pair_token, mode="drop")
    slot_gate = jnp.zeros((n_blocks, EXPERTS * CAPACITY), jnp.float32).at[block_ids, dest_row].set(gate.reshape(n_blocks, TOK_DEV * TOP_K), mode="drop")
    src_by_exp = src_tok.reshape(n_blocks, EXPERTS, CAPACITY).transpose(1, 0, 2)
    gate_by_exp = slot_gate.reshape(n_blocks, EXPERTS, CAPACITY).transpose(1, 0, 2)

    def expert_step(running, inputs):
        src_e, gate_e, wg_e, wu_e, wd_e = inputs
        expert_rows = jax.vmap(take_rows)(x_blocks, src_e).reshape(n_blocks * CAPACITY, D_MODEL)
        gate_act = jnp.dot(expert_rows, wg_e, preferred_element_type=jnp.float32)
        up_act = jnp.dot(expert_rows, wu_e, preferred_element_type=jnp.float32)
        hidden = (jax.nn.silu(gate_act) * up_act).astype(jnp.bfloat16)
        out_rows = jnp.dot(hidden, wd_e, preferred_element_type=jnp.float32).astype(jnp.bfloat16)
        contrib = out_rows.reshape(n_blocks, CAPACITY, D_MODEL).astype(jnp.float32) * gate_e[:, :, None]
        return running.at[block_ids, src_e].add(contrib, mode="drop"), None

    summed = lax.scan(expert_step, x_blocks.astype(jnp.float32), (src_by_exp, gate_by_exp, w_gate, w_up, w_down))[0]
    return summed.astype(jnp.bfloat16).reshape(n_blocks * TOK_DEV, D_MODEL)
```

```python
import functools

import jax
import jax.numpy as jnp
from jax import lax
from jax.experimental import pallas as pl
from jax.experimental.pallas import tpu as pltpu
from jax.sharding import PartitionSpec as P


BF16 = jnp.bfloat16
F32 = jnp.float32
I32 = jnp.int32
VMEM_LIMIT = 66_000_000

TILE = 256
TOK_BLOCK = 256
MIX_TILE = 128
ALIGN = 16
SLAB = MIX_TILE + ALIGN
SUB = 512
WIDE_CHUNKS = (1024, 1536, 1536, 1536)
DOWN_PIECES = (512, 256, 256)


def capacity_rows(tok_rows, top_k, n_exp):
    return max(8, ((5 * top_k * tok_rows) // (4 * n_exp) + 7) // 8 * 8)


def after(value, *earlier):
    return lax.optimization_barrier((value, earlier))[0]


def any_spec():
    return pl.BlockSpec(memory_space=pl.ANY)


def pack_body(n_local, local, n_blk, n_group, first_ref, slot_ref, x_ref, *refs):
    out_refs, acc_ref = refs[:n_group], refs[n_group]
    e, s = pl.program_id(0) * n_local + local, pl.program_id(1)
    count = first_ref[e * (n_blk + 1) + n_blk]
    base = s * TILE

    @pl.when(base < count)
    def _():
        end = jnp.minimum(base + TILE, count)
        lo = jnp.int32(0)
        hi = jnp.int32(0)
        for i in range(n_blk):
            lo += (first_ref[e * (n_blk + 1) + i + 1] <= base).astype(I32)
            hi += (first_ref[e * (n_blk + 1) + i] < end).astype(I32)
        acc_ref[...] = jnp.zeros_like(acc_ref)
        slots = base + lax.broadcasted_iota(I32, (TILE, TOK_BLOCK), 0)

        def visit(i, carry):
            off = pl.multiple_of(i * TOK_BLOCK, TOK_BLOCK)
            pick = (slots == slot_ref[pl.ds(e, 1), pl.ds(off, TOK_BLOCK)]).astype(F32).astype(BF16)
            acc_ref[...] += jnp.dot(pick, x_ref[pl.ds(off, TOK_BLOCK), :], preferred_element_type=F32)
            return carry

        lax.fori_loop(lo, hi, visit, 0)
        for d in range(n_group):

            @pl.when(pl.program_id(0) == d)
            def _():
                out_refs[d][...] = acc_ref[...].astype(BF16)


def pack_rows(first_blk, x_loc, slot_te, n_exp, n_local, local, capacity):
    tok_rows, d_model = x_loc.shape
    n_blk = tok_rows // TOK_BLOCK
    n_group = n_exp // n_local

    def out_spec(d):
        def index(p, s, first):
            used = (first[(d * n_local + local) * (n_blk + 1) + n_blk] + TILE - 1) // TILE
            last = jnp.maximum(used - 1, 0)
            return jnp.where(p < d, 0, jnp.where(p > d, last, jnp.minimum(s, last))), 0

        return pl.BlockSpec((TILE, d_model), index)

    return pl.pallas_call(
        functools.partial(pack_body, n_local, local, n_blk, n_group),
        grid_spec=pltpu.PrefetchScalarGridSpec(
            num_scalar_prefetch=1,
            grid=(n_group, capacity // TILE),
            in_specs=[
                pl.BlockSpec((n_exp, tok_rows), lambda p, s, f: (0, 0)),
                pl.BlockSpec((tok_rows, d_model), lambda p, s, f: (0, 0)),
            ],
            out_specs=[out_spec(d) for d in range(n_group)],
            scratch_shapes=[pltpu.VMEM((TILE, d_model), F32)],
        ),
        out_shape=[jax.ShapeDtypeStruct((capacity, d_model), BF16)] * n_group,
        compiler_params=pltpu.CompilerParams(vmem_limit_bytes=VMEM_LIMIT),
        cost_estimate=pl.CostEstimate(flops=20_000_000_000, bytes_accessed=60_000_000, transcendentals=0),
        name="pack_rows",
    )(first_blk, slot_te, x_loc)


def wide_body(n_group, local, lo_col, cols, meta_ref, *refs):
    x_refs = refs[:n_group]
    wg_ref, wu_ref, far_ref, h_ref, rows_buf, gate_w, up_w, row_sems, sems = refs[n_group:]
    side = meta_ref[0]
    half = wg_ref.shape[1]
    i = pl.program_id(0)
    n_live = meta_ref[1 + n_group]

    def fetch(step):
        for d in range(n_group):

            @pl.when((step >= meta_ref[1 + d]) & (step < meta_ref[2 + d]))
            def _():
                at = pl.multiple_of((step - meta_ref[1 + d]) * TILE, TILE)
                pltpu.make_async_copy(x_refs[d].at[pl.ds(at, TILE), :], rows_buf.at[step % 2], row_sems.at[step % 2]).start()

    @pl.when(i == 0)
    def _():
        fetch(i)
        near = pl.ds(pl.multiple_of(side * half, half), half)
        far = pl.ds(pl.multiple_of((1 - side) * half, half), half)
        copies = [
            pltpu.make_async_copy(wg_ref.at[local, :, pl.ds(lo_col, cols)], gate_w.at[near, :], sems.at[0]),
            pltpu.make_async_copy(wu_ref.at[local, :, pl.ds(lo_col, cols)], up_w.at[near, :], sems.at[1]),
            pltpu.make_async_copy(far_ref.at[0], gate_w.at[far, :], sems.at[2]),
            pltpu.make_async_copy(far_ref.at[1], up_w.at[far, :], sems.at[3]),
        ]
        for copy in copies:
            copy.start()
        for copy in copies:
            copy.wait()

    @pl.when(i < n_live)
    def _():
        fetch(i + 1)
        pltpu.make_async_copy(x_refs[0].at[pl.ds(0, TILE), :], rows_buf.at[i % 2], row_sems.at[i % 2]).wait()
        rows = rows_buf[i % 2]
        for j in range(0, cols, SUB):
            g = jnp.dot(rows, gate_w[:, j : j + SUB], preferred_element_type=F32)
            u = jnp.dot(rows, up_w[:, j : j + SUB], preferred_element_type=F32)
            h_ref[:, j : j + SUB] = (jax.nn.silu(g) * u).astype(BF16)


def wide_part(meta, rows, w_gate, w_up, far, local, lo_col, cols):
    n_group = len(rows)
    capacity, d_model = rows[0].shape
    n_rows = n_group * capacity
    return pl.pallas_call(
        functools.partial(wide_body, n_group, local, lo_col, cols),
        grid_spec=pltpu.PrefetchScalarGridSpec(
            num_scalar_prefetch=1,
            grid=(n_rows // TILE,),
            in_specs=[any_spec()] * (n_group + 3),
            out_specs=pl.BlockSpec((TILE, cols), lambda i, m: (jnp.clip(i, 0, jnp.maximum(m[1 + n_group] - 1, 0)), 0)),
            scratch_shapes=[
                pltpu.VMEM((2, TILE, d_model), BF16),
                pltpu.VMEM((d_model, cols), BF16),
                pltpu.VMEM((d_model, cols), BF16),
                pltpu.SemaphoreType.DMA((2,)),
                pltpu.SemaphoreType.DMA((4,)),
            ],
        ),
        out_shape=jax.ShapeDtypeStruct((n_rows, cols), BF16),
        compiler_params=pltpu.CompilerParams(vmem_limit_bytes=VMEM_LIMIT),
        cost_estimate=pl.CostEstimate(flops=4 * n_rows * d_model * cols, bytes_accessed=n_rows * d_model * 2, transcendentals=0),
        name="wide_part",
    )(meta, *rows, w_gate, w_up, far)


def down_body(n_group, splits, local, meta_ref, *refs):
    h_refs = refs[: len(splits)]
    w_ref = refs[len(splits)]
    out_refs = refs[len(splits) + 1 : len(splits) + 1 + n_group]
    w_buf, sem = refs[-2:]
    i = pl.program_id(0)

    @pl.when(i == 0)
    def _():
        copy = pltpu.make_async_copy(w_ref if local is None else w_ref.at[local], w_buf, sem)
        copy.start()
        copy.wait()

    @pl.when(i < meta_ref[1 + n_group])
    def _():
        total = None
        lo = 0
        for h_ref, cols in zip(h_refs, splits):
            part = jnp.dot(h_ref[...], w_buf[lo : lo + cols, :], preferred_element_type=F32)
            total = part if total is None else total + part
            lo += cols
        total = total.astype(BF16)
        for d in range(n_group):

            @pl.when((i >= meta_ref[1 + d]) & (i < meta_ref[2 + d]))
            def _():
                out_refs[d][...] = total


def down_part(meta, hidden, weight, n_group, local=None):
    n_rows = hidden[0].shape[0]
    splits = tuple(h.shape[1] for h in hidden)
    ffn, width = weight.shape[-2:]

    def h_spec(w):
        return pl.BlockSpec((TILE, w), lambda i, m: (jnp.clip(i, 0, jnp.maximum(m[1 + n_group] - 1, 0)), 0))

    def out_spec(d):
        def index(i, m):
            return jnp.clip(i - m[1 + d], 0, jnp.maximum(m[2 + d] - m[1 + d] - 1, 0)), 0

        return pl.BlockSpec((TILE, width), index)

    return pl.pallas_call(
        functools.partial(down_body, n_group, splits, local),
        grid_spec=pltpu.PrefetchScalarGridSpec(
            num_scalar_prefetch=1,
            grid=(n_rows // TILE,),
            in_specs=[h_spec(cols) for cols in splits] + [any_spec()],
            out_specs=[out_spec(d) for d in range(n_group)],
            scratch_shapes=[pltpu.VMEM((ffn, width), BF16), pltpu.SemaphoreType.DMA],
        ),
        out_shape=[jax.ShapeDtypeStruct((n_rows // n_group, width), BF16)] * n_group,
        compiler_params=pltpu.CompilerParams(vmem_limit_bytes=VMEM_LIMIT),
        cost_estimate=pl.CostEstimate(flops=2 * n_rows * ffn * width, bytes_accessed=n_rows * ffn * 2, transcendentals=0),
        name="down_part",
    )(meta, *hidden, weight)


def slab_start(first, e, n_tile, i, capacity):
    return jnp.minimum(first[e * n_tile + i] // ALIGN * ALIGN, capacity - SLAB)


def mix_body(n_exp, n_tile, capacity, with_pick, col_ref, first_ref, count_ref, pos_ref, gate_ref, x_ref, *refs):
    back_refs, refs = refs[:n_exp], refs[n_exp:]
    pick_ref = refs[0] if with_pick else refs[-1]
    y_ref, mark_ref = refs[-2:] if with_pick else refs[-3:-1]
    i = pl.program_id(0)
    reach = n_exp * SLAB
    if not with_pick:
        col = lax.broadcasted_iota(I32, (MIX_TILE, reach), 1)
        for j in range(2):
            pick_ref[:, j * reach : (j + 1) * reach] = (col == pos_ref[:, j : j + 1]).astype(F32).astype(BF16)
    row = lax.broadcasted_iota(I32, (SLAB, 1), 0)
    parts = []
    for e in range(n_exp):
        start = slab_start(first_ref, e, n_tile, i, capacity)
        slab = back_refs[e][pl.ds(pl.multiple_of(start, ALIGN), SLAB), :]
        parts.append(jnp.where(row + start < count_ref[e], slab, jnp.zeros_like(slab)))
    rows = jnp.concatenate(parts, axis=0)
    o0 = jnp.dot(pick_ref[:, :reach], rows, preferred_element_type=F32)
    o1 = jnp.dot(pick_ref[:, reach:], rows, preferred_element_type=F32)
    mixed = gate_ref[:, 0:1] * o0 + gate_ref[:, 1:2] * o1
    y_ref[...] = (x_ref[...].astype(F32) + mixed).astype(BF16)
    mark_ref[...] = jnp.zeros_like(mark_ref)


def mix_cols(col_block, y_loc, pick, x_loc, pos, gate_loc, first_mix, counts, back):
    tok_rows, d_model = x_loc.shape
    n_tile = tok_rows // MIX_TILE
    n_exp = len(back)
    capacity, width = back[0].shape
    reach = n_exp * SLAB
    tile = lambda w: pl.BlockSpec((MIX_TILE, w), lambda i, c, f, n: (i, 0))
    cols = pl.BlockSpec((MIX_TILE, width), lambda i, c, f, n: (i, c[0]))
    mark = pl.BlockSpec((8, 128), lambda i, c, f, n: (0, 0))
    whole = pl.BlockSpec((capacity, width), lambda i, c, f, n: (0, 0))
    args = [col_block, first_mix, counts, pos, gate_loc, x_loc, *back]
    specs = [tile(2), tile(2), cols] + [whole] * n_exp
    outs = [jax.ShapeDtypeStruct((tok_rows, d_model), BF16), jax.ShapeDtypeStruct((8, 128), I32)]
    out_specs = [cols, mark]
    alias = {}
    if pick is None:
        outs.append(jax.ShapeDtypeStruct((tok_rows, 2 * reach), BF16))
        out_specs.append(tile(2 * reach))
    else:
        args += [pick, y_loc]
        specs += [tile(2 * reach), any_spec()]
        alias = {len(args) - 1: 0}
    return pl.pallas_call(
        functools.partial(mix_body, n_exp, n_tile, capacity, pick is not None),
        grid_spec=pltpu.PrefetchScalarGridSpec(num_scalar_prefetch=3, grid=(n_tile,), in_specs=specs, out_specs=out_specs),
        out_shape=outs,
        input_output_aliases=alias,
        compiler_params=pltpu.CompilerParams(vmem_limit_bytes=VMEM_LIMIT),
        cost_estimate=pl.CostEstimate(flops=20_000_000 * width, bytes_accessed=20_000 * width, transcendentals=0),
        name="mix_cols",
    )(*args)


def spans(sizes):
    lo = 0
    for size in sizes:
        yield lo, size
        lo += size


def solution(mesh):
    n_group, n_side = mesh.shape["expert"], mesh.shape["data"]
    tok_spec = P(("rep", "expert", "data"), None)
    wide_spec = P("expert", "data", None)
    down_spec = P("expert", None, "data")
    swap = [(s, 1 - s) for s in range(n_side)]

    def whole_step(x_loc, idx_loc, gate_loc, wg_loc, wu_loc, wd_loc):
        tok_rows, _ = x_loc.shape
        top_k = idx_loc.shape[1]
        n_local, half, _ = wg_loc.shape
        n_exp = n_local * n_group
        capacity = capacity_rows(tok_rows, top_k, n_exp)
        side = lax.axis_index("data")
        place = lax.axis_index("expert")
        locals_ = range(n_local)
        groups = jnp.arange(n_group, dtype=I32)

        ids = ((idx_loc // n_local + n_group - place) % n_group * n_local + idx_loc % n_local).T
        experts = jnp.arange(n_exp, dtype=I32)[:, None]
        chosen = functools.reduce(jnp.logical_or, [ids[j][None, :] == experts for j in range(top_k)])
        chosen_i = chosen.astype(I32)
        running = jnp.cumsum(chosen_i, axis=1)
        before = running - chosen_i
        slot_te = jnp.where(chosen & (before < capacity), before, -1)
        counts = jnp.minimum(running[:, -1], capacity)
        first = jnp.minimum(before, capacity)
        first_blk = jnp.concatenate([first[:, ::TOK_BLOCK], counts[:, None]], axis=1).reshape(-1)
        first_mix = first[:, ::MIX_TILE]

        table = lax.all_gather(counts, "expert")
        meta = []
        for l in locals_:
            mine = jnp.sum(jnp.where(((place - groups) % n_group)[:, None, None] == groups[None, :, None], table.reshape(n_group, n_group, n_local)[None, :, :, l] * (groups[:, None, None] == groups[None, None, :]), 0), axis=(1, 2))
            ends = jnp.cumsum((mine + TILE - 1) // TILE)
            meta.append(jnp.concatenate([side[None], jnp.zeros((1,), I32), ends]).astype(I32))

        starts = jnp.minimum(first_mix // ALIGN * ALIGN, capacity - SLAB)
        at = jnp.where(slot_te < 0, -n_exp * SLAB, slot_te - jnp.repeat(starts, MIX_TILE, axis=1) + experts * SLAB)
        pos = jnp.stack([jnp.sum(jnp.where(ids[j][None, :] == experts, at, 0), axis=0) for j in range(top_k)], axis=1)
        first_mix = first_mix.reshape(-1)

        done = []

        def in_turn(kernel, small, *args):
            if done:
                small = after(small, done[-1]) if done[-1].ndim else small + done[-1]
            out = kernel(small, *args)
            done.append(out[0] if isinstance(out, (list, tuple)) else out)
            return out

        wide_spans = list(spans(WIDE_CHUNKS))
        down_spans = list(spans(DOWN_PIECES))
        parts = [jnp.stack([w[l, :, lo : lo + n] for w in (wg_loc, wu_loc)]) for l in locals_ for lo, n in wide_spans]
        parts += [wd_loc[l, :, lo : lo + n] for lo, n in down_spans for l in locals_]
        far = []

        def cross():
            if len(far) == len(parts):
                return
            piece = parts[len(far)]
            if len(far) >= 2:
                piece = after(piece, far[-2])
            far.append(lax.ppermute(piece, "data", swap))

        def exchange(blocks, step):
            out = [blocks[0]]
            for d in range(1, n_group):
                out.append(lax.ppermute(blocks[d], "expert", [(s, (s + step * d) % n_group) for s in range(n_group)]))
            return out

        def mix(y_loc, pick, col_block, back):
            back = [back[l][d] for d in range(n_group) for l in locals_]
            out = in_turn(mix_cols, col_block.astype(I32)[None], y_loc, pick, x_loc, pos, gate_loc, first_mix, counts, back)
            done[-1] = out[1][0, 0]
            return out[0], out[2] if pick is None else pick

        cross()
        cross()
        first_blk = after(first_blk, meta)
        rows = [exchange(in_turn(pack_rows, first_blk, x_loc, slot_te, n_exp, n_local, 0, capacity), 1)]
        cross()
        packed = in_turn(pack_rows, first_blk, x_loc, slot_te, n_exp, n_local, 1, capacity)
        cross()
        rows.append(exchange([after(block, rows[0]) for block in packed], 1))

        n_wide = len(wide_spans)
        hidden, own = [], []
        for l in locals_:
            hidden.append([])
            for k, (lo, n) in enumerate(wide_spans):
                if l or k >= 2:
                    cross()
                hidden[l].append(in_turn(wide_part, meta[l], rows[l], wg_loc, wu_loc, far[l * n_wide + k], l, lo, n))
            own.append(exchange(in_turn(down_part, meta[l], hidden[l], wd_loc, n_group, l), -1))

        def far_piece(c, l):
            cross()
            return exchange(in_turn(down_part, meta[l], hidden[l], far[n_local * (n_wide + c) + l], n_group), -1)

        def col_block(c):
            return ((1 - side) * half + down_spans[c][0]) // down_spans[c][1]

        piece = [far_piece(0, l) for l in locals_]
        y_loc, pick = mix(None, None, side, own)
        for c in range(1, len(down_spans) - 1):
            piece, ready = [far_piece(c, l) for l in locals_], piece
            y_loc, pick = mix(y_loc, pick, col_block(c - 1), ready)
        c = len(down_spans) - 1
        last = [far_piece(c, 0)]
        y_loc, pick = mix(y_loc, pick, col_block(c - 1), piece)
        last.append(far_piece(c, 1))
        return mix(y_loc, pick, col_block(c), last)[0]

    in_specs = (tok_spec, tok_spec, tok_spec, wide_spec, wide_spec, down_spec)
    return jax.shard_map(whole_step, mesh=mesh, in_specs=in_specs, out_specs=tok_spec, check_vma=False)
```

```python
import functools

import jax
import jax.numpy as jnp
from jax import lax
from jax.experimental import pallas as pl
from jax.experimental.pallas import tpu as pltpu
from jax.sharding import PartitionSpec as P


BF16 = jnp.bfloat16
F32 = jnp.float32
I32 = jnp.int32
VMEM_LIMIT = 66_000_000

TILE = 256
TOK_BLOCK = 256
MIX_TILE = 128
MIX_UNROLL = 4
ALIGN = 16
REACH = 512
DEEP = 4
SUB = 512
WIDE_CHUNKS = (512, 1536, 1536, 2048)
DOWN_PIECES = ((0, 0, 512), (1, 0, 512), (0, 512, 256), (1, 512, 256), (0, 768, 256), (1, 768, 128), (1, 896, 128))


def capacity_rows(tok_rows, top_k, n_exp):
    return max(8, ((5 * top_k * tok_rows) // (4 * n_exp) + 7) // 8 * 8)


def after(value, *earlier):
    return lax.optimization_barrier((value, earlier))[0]


def any_spec():
    return pl.BlockSpec(memory_space=pl.ANY)


def pack_body(n_local, local, n_blk, n_group, first_ref, slot_ref, x_ref, *refs):
    out_refs, acc_ref = refs[:n_group], refs[n_group]
    e, s = pl.program_id(0) * n_local + local, pl.program_id(1)
    count = first_ref[e * (n_blk + 1) + n_blk]
    base = s * TILE

    @pl.when(base < count)
    def _():
        end = jnp.minimum(base + TILE, count)
        lo = jnp.int32(0)
        hi = jnp.int32(0)
        for i in range(n_blk):
            lo += (first_ref[e * (n_blk + 1) + i + 1] <= base).astype(I32)
            hi += (first_ref[e * (n_blk + 1) + i] < end).astype(I32)
        acc_ref[...] = jnp.zeros_like(acc_ref)
        slots = base + lax.broadcasted_iota(I32, (TILE, TOK_BLOCK), 0)

        def visit(i, carry):
            off = pl.multiple_of(i * TOK_BLOCK, TOK_BLOCK)
            pick = (slots == slot_ref[pl.ds(e, 1), pl.ds(off, TOK_BLOCK)]).astype(F32).astype(BF16)
            acc_ref[...] += jnp.dot(pick, x_ref[pl.ds(off, TOK_BLOCK), :], preferred_element_type=F32)
            return carry

        lax.fori_loop(lo, hi, visit, 0)
        for d in range(n_group):

            @pl.when(pl.program_id(0) == d)
            def _():
                out_refs[d][...] = acc_ref[...].astype(BF16)


def pack_rows(first_blk, x_loc, slot_te, n_exp, n_local, local, capacity):
    tok_rows, d_model = x_loc.shape
    n_blk = tok_rows // TOK_BLOCK
    n_group = n_exp // n_local

    def out_spec(d):
        def index(p, s, first):
            used = (first[(d * n_local + local) * (n_blk + 1) + n_blk] + TILE - 1) // TILE
            last = jnp.maximum(used - 1, 0)
            return jnp.where(p < d, 0, jnp.where(p > d, last, jnp.minimum(s, last))), 0

        return pl.BlockSpec((TILE, d_model), index)

    return pl.pallas_call(
        functools.partial(pack_body, n_local, local, n_blk, n_group),
        grid_spec=pltpu.PrefetchScalarGridSpec(
            num_scalar_prefetch=1,
            grid=(n_group, capacity // TILE),
            in_specs=[
                pl.BlockSpec((n_exp, tok_rows), lambda p, s, f: (0, 0)),
                pl.BlockSpec((tok_rows, d_model), lambda p, s, f: (0, 0)),
            ],
            out_specs=[out_spec(d) for d in range(n_group)],
            scratch_shapes=[pltpu.VMEM((TILE, d_model), F32)],
        ),
        out_shape=[jax.ShapeDtypeStruct((capacity, d_model), BF16)] * n_group,
        compiler_params=pltpu.CompilerParams(vmem_limit_bytes=VMEM_LIMIT),
        cost_estimate=pl.CostEstimate(flops=20_000_000_000, bytes_accessed=60_000_000, transcendentals=0),
        name="pack_rows",
    )(first_blk, slot_te, x_loc)


def smem():
    return pl.BlockSpec(memory_space=pltpu.SMEM)


def tile_at(i):
    return pl.ds(pl.multiple_of(i * TILE, TILE), TILE)


def wide_body(n_group, local, lo_col, cols, meta_ref, *refs):
    x_refs = refs[:n_group]
    wg_ref, wu_ref, far_ref = refs[n_group : n_group + 3]
    h_ref, rows_buf, h_buf, gate_w, up_w, row_sems, h_sems, sems = refs[-8:]
    side = meta_ref[0]
    half = wg_ref.shape[1]
    n_live = meta_ref[1 + n_group]

    def fetch(i):
        for d in range(n_group):

            @pl.when((i >= meta_ref[1 + d]) & (i < meta_ref[2 + d]))
            def _():
                pltpu.make_async_copy(x_refs[d].at[tile_at(i - meta_ref[1 + d]), :], rows_buf.at[i % 2], row_sems.at[i % 2]).start()

    def send(i):
        return pltpu.make_async_copy(h_buf.at[i % 2], h_ref.at[tile_at(i), pl.ds(lo_col, cols)], h_sems.at[i % 2])

    fetch(0)
    near = pl.ds(pl.multiple_of(side * half, half), half)
    far = pl.ds(pl.multiple_of((1 - side) * half, half), half)
    copies = [
        pltpu.make_async_copy(wg_ref.at[local, :, pl.ds(lo_col, cols)], gate_w.at[near, :], sems.at[0]),
        pltpu.make_async_copy(wu_ref.at[local, :, pl.ds(lo_col, cols)], up_w.at[near, :], sems.at[1]),
        pltpu.make_async_copy(far_ref.at[0], gate_w.at[far, :], sems.at[2]),
        pltpu.make_async_copy(far_ref.at[1], up_w.at[far, :], sems.at[3]),
    ]
    for copy in copies:
        copy.start()
    for copy in copies:
        copy.wait()

    def step(i, carry):
        fetch(i + 1)
        pltpu.make_async_copy(x_refs[0].at[tile_at(0), :], rows_buf.at[i % 2], row_sems.at[i % 2]).wait()

        @pl.when(i >= 2)
        def _():
            send(i - 2).wait()

        rows = rows_buf[i % 2]
        for j in range(0, cols, SUB):
            g = jnp.dot(rows, gate_w[:, j : j + SUB], preferred_element_type=F32)
            u = jnp.dot(rows, up_w[:, j : j + SUB], preferred_element_type=F32)
            h_buf[i % 2, :, j : j + SUB] = (jax.nn.silu(g) * u).astype(BF16)
        send(i).start()
        return carry

    lax.fori_loop(0, n_live, step, 0)
    for back in (2, 1):

        @pl.when(n_live >= back)
        def _():
            send(n_live - back).wait()


def wide_part(meta, hidden, rows, w_gate, w_up, far, local, lo_col, cols):
    n_group = len(rows)
    capacity, d_model = rows[0].shape
    n_rows = n_group * capacity
    ffn = w_gate.shape[2]
    args = [meta, *rows, w_gate, w_up, far]
    alias = {}
    if hidden is not None:
        alias = {len(args): 0}
        args.append(hidden)
    return pl.pallas_call(
        functools.partial(wide_body, n_group, local, lo_col, cols),
        in_specs=[smem()] + [any_spec()] * (len(args) - 1),
        out_specs=any_spec(),
        scratch_shapes=[
            pltpu.VMEM((2, TILE, d_model), BF16),
            pltpu.VMEM((2, TILE, cols), BF16),
            pltpu.VMEM((d_model, cols), BF16),
            pltpu.VMEM((d_model, cols), BF16),
            pltpu.SemaphoreType.DMA((2,)),
            pltpu.SemaphoreType.DMA((2,)),
            pltpu.SemaphoreType.DMA((4,)),
        ],
        out_shape=jax.ShapeDtypeStruct((n_rows, ffn), BF16),
        input_output_aliases=alias,
        compiler_params=pltpu.CompilerParams(vmem_limit_bytes=VMEM_LIMIT),
        cost_estimate=pl.CostEstimate(flops=4 * n_rows * d_model * cols, bytes_accessed=n_rows * d_model * 2, transcendentals=0),
        name="wide_part",
    )(*args)


def down_body(n_group, local, meta_ref, h_ref, w_ref, *refs):
    out_refs = refs[:n_group]
    h_buf, out_buf, w_buf, h_sems, out_sems, sem = refs[n_group:]
    n_live = meta_ref[1 + n_group]

    def fetch(i):
        return pltpu.make_async_copy(h_ref.at[tile_at(i), :], h_buf.at[i % DEEP], h_sems.at[i % DEEP])

    def sent(i):
        pltpu.make_async_copy(out_buf.at[i % 2], out_refs[0].at[tile_at(0), :], out_sems.at[i % 2]).wait()

    for i in range(DEEP - 1):

        @pl.when(i < n_live)
        def _():
            fetch(i).start()

    copy = pltpu.make_async_copy(w_ref if local is None else w_ref.at[local], w_buf, sem)
    copy.start()
    copy.wait()

    def step(i, carry):
        @pl.when(i + DEEP - 1 < n_live)
        def _():
            fetch(i + DEEP - 1).start()

        fetch(i).wait()

        @pl.when(i >= 2)
        def _():
            sent(i)

        out_buf[i % 2] = jnp.dot(h_buf[i % DEEP], w_buf[...], preferred_element_type=F32).astype(BF16)
        for d in range(n_group):

            @pl.when((i >= meta_ref[1 + d]) & (i < meta_ref[2 + d]))
            def _():
                pltpu.make_async_copy(out_buf.at[i % 2], out_refs[d].at[tile_at(i - meta_ref[1 + d]), :], out_sems.at[i % 2]).start()

        return carry

    lax.fori_loop(0, n_live, step, 0)
    for back in (2, 1):

        @pl.when(n_live >= back)
        def _():
            sent(n_live - back)

    for d in range(n_group):
        @pl.when(meta_ref[1 + d] == meta_ref[2 + d])
        def _():
            out_buf[0] = jnp.zeros_like(out_buf[0])
            blank = pltpu.make_async_copy(out_buf.at[0], out_refs[d].at[tile_at(0), :], out_sems.at[0])
            blank.start()
            blank.wait()


def down_part(meta, hidden, weight, n_group, local=None):
    n_rows = hidden.shape[0]
    ffn, width = weight.shape[-2:]
    return pl.pallas_call(
        functools.partial(down_body, n_group, local),
        in_specs=[smem(), any_spec(), any_spec()],
        out_specs=[any_spec()] * n_group,
        scratch_shapes=[
            pltpu.VMEM((DEEP, TILE, ffn), BF16),
            pltpu.VMEM((2, TILE, width), BF16),
            pltpu.VMEM((ffn, width), BF16),
            pltpu.SemaphoreType.DMA((DEEP,)),
            pltpu.SemaphoreType.DMA((2,)),
            pltpu.SemaphoreType.DMA,
        ],
        out_shape=[jax.ShapeDtypeStruct((n_rows // n_group, width), BF16)] * n_group,
        compiler_params=pltpu.CompilerParams(vmem_limit_bytes=VMEM_LIMIT),
        cost_estimate=pl.CostEstimate(flops=2 * n_rows * ffn * width, bytes_accessed=n_rows * ffn * 2, transcendentals=0),
        name="down_part",
    )(meta, hidden, weight)


def mix_body(n_exp, n_tile, subs, col_ref, chunk_ref, pos_ref, gate_ref, x_ref, *refs):
    back_refs = refs[:n_exp]
    y_ref, mark_ref, back_buf, near_buf, x_buf, y_buf, sems = refs[-7:]
    width = x_buf.shape[1]
    capacity = back_refs[0].shape[0]
    cols = pl.ds(pl.multiple_of(col_ref[0], 128), width)
    copies = [
        pltpu.make_async_copy(ref.at[:, pl.ds(sub * width, width)], back_buf.at[pl.ds(e * capacity, capacity), :], sems.at[e])
        for e, (ref, sub) in enumerate(zip(back_refs, subs))
    ]
    copies.append(pltpu.make_async_copy(x_ref.at[:, cols], x_buf, sems.at[n_exp]))
    for copy in copies:
        copy.start()
    for copy in copies:
        copy.wait()

    def step(block, carry):
        for k in range(MIX_UNROLL):
            i = block * MIX_UNROLL + k
            tokens = pl.ds(pl.multiple_of(i * MIX_TILE, MIX_TILE), MIX_TILE)
            for c in range(REACH // ALIGN):
                chunk = pl.multiple_of(chunk_ref[i * (REACH // ALIGN) + c], ALIGN)
                near_buf[k, c * ALIGN : (c + 1) * ALIGN, :] = back_buf[pl.ds(chunk, ALIGN), :]
            seat = lax.broadcasted_iota(I32, (MIX_TILE, REACH), 1)
            pick = jnp.concatenate([(seat == pos_ref[tokens, j : j + 1]).astype(F32).astype(BF16) for j in range(2)], axis=0)
            found = jnp.dot(pick, near_buf[k], preferred_element_type=F32)
            mixed = gate_ref[tokens, 0:1] * found[:MIX_TILE] + gate_ref[tokens, 1:2] * found[MIX_TILE:]
            y_buf[tokens, :] = (x_buf[tokens, :].astype(F32) + mixed).astype(BF16)
        return carry

    lax.fori_loop(0, n_tile // MIX_UNROLL, step, 0)
    out = pltpu.make_async_copy(y_buf, y_ref.at[:, cols], sems.at[0])
    out.start()
    out.wait()
    mark_ref[0] = 0


def mix_cols(col, y_loc, x_loc, pos, gate_loc, chunks, width, back):
    tok_rows, d_model = x_loc.shape
    n_exp = len(back)
    capacity = back[0][0].shape[0]
    vmem = pl.BlockSpec(memory_space=pltpu.VMEM)
    args = [col, chunks, pos, gate_loc, x_loc, *[array for array, _ in back]]
    specs = [smem(), smem(), vmem, vmem, any_spec()] + [any_spec()] * n_exp
    alias = {}
    if y_loc is not None:
        alias = {len(args): 0}
        args.append(y_loc)
        specs.append(any_spec())
    return pl.pallas_call(
        functools.partial(mix_body, n_exp, tok_rows // MIX_TILE, tuple(sub for _, sub in back)),
        in_specs=specs,
        out_specs=[any_spec(), smem()],
        scratch_shapes=[
            pltpu.VMEM((n_exp * capacity, width), BF16),
            pltpu.VMEM((MIX_UNROLL, REACH, width), BF16),
            pltpu.VMEM((tok_rows, width), BF16),
            pltpu.VMEM((tok_rows, width), BF16),
            pltpu.SemaphoreType.DMA((n_exp + 1,)),
        ],
        out_shape=[jax.ShapeDtypeStruct((tok_rows, d_model), BF16), jax.ShapeDtypeStruct((1,), I32)],
        input_output_aliases=alias,
        compiler_params=pltpu.CompilerParams(vmem_limit_bytes=VMEM_LIMIT),
        cost_estimate=pl.CostEstimate(flops=20_000_000 * width, bytes_accessed=20_000 * width, transcendentals=0),
        name="mix_cols",
    )(*args)


def spans(sizes):
    lo = 0
    for size in sizes:
        yield lo, size
        lo += size


def solution(mesh):
    n_group, n_side = mesh.shape["expert"], mesh.shape["data"]
    tok_spec = P(("rep", "expert", "data"), None)
    wide_spec = P("expert", "data", None)
    down_spec = P("expert", None, "data")
    swap = [(s, 1 - s) for s in range(n_side)]

    def whole_step(x_loc, idx_loc, gate_loc, wg_loc, wu_loc, wd_loc):
        tok_rows, _ = x_loc.shape
        top_k = idx_loc.shape[1]
        n_local, half, _ = wg_loc.shape
        n_exp = n_local * n_group
        capacity = capacity_rows(tok_rows, top_k, n_exp)
        side = lax.axis_index("data")
        place = lax.axis_index("expert")
        locals_ = range(n_local)
        groups = jnp.arange(n_group, dtype=I32)

        ids = ((idx_loc // n_local + n_group - place) % n_group * n_local + idx_loc % n_local).T
        experts = jnp.arange(n_exp, dtype=I32)[:, None]
        chosen = functools.reduce(jnp.logical_or, [ids[j][None, :] == experts for j in range(top_k)])
        chosen_i = chosen.astype(I32)
        running = jnp.cumsum(chosen_i, axis=1)
        before = running - chosen_i
        slot_te = jnp.where(chosen & (before < capacity), before, -1)
        counts = jnp.minimum(running[:, -1], capacity)
        first = jnp.minimum(before, capacity)
        first_blk = jnp.concatenate([first[:, ::TOK_BLOCK], counts[:, None]], axis=1).reshape(-1)
        first_mix = first[:, ::MIX_TILE]

        table = lax.all_gather(counts, "expert")
        meta = []
        for l in locals_:
            mine = jnp.sum(jnp.where(((place - groups) % n_group)[:, None, None] == groups[None, :, None], table.reshape(n_group, n_group, n_local)[None, :, :, l] * (groups[:, None, None] == groups[None, None, :]), 0), axis=(1, 2))
            ends = jnp.cumsum((mine + TILE - 1) // TILE)
            meta.append(jnp.concatenate([side[None], jnp.zeros((1,), I32), ends]).astype(I32))

        reach = REACH // ALIGN
        start = first_mix // ALIGN
        stop = jnp.concatenate([first_mix[:, 1:], counts[:, None]], axis=1)
        size = jnp.where(stop > first_mix, (stop + ALIGN - 1) // ALIGN - start, 0)
        lead = jnp.cumsum(size, axis=0) - size
        at = slot_te + jnp.repeat((lead - start) * ALIGN, MIX_TILE, axis=1)
        at = jnp.where(slot_te < 0, -1, at)
        pos = jnp.stack([jnp.sum(jnp.where(ids[j][None, :] == experts, at, 0), axis=0) for j in range(top_k)], axis=1)
        seat = jnp.arange(reach, dtype=I32)[None, None, :]
        taken = (seat >= lead[:, :, None]) & (seat < (lead + size)[:, :, None])
        source = experts[:, :, None] * (capacity // ALIGN) + (start - lead)[:, :, None] + seat
        chunks = (jnp.sum(jnp.where(taken, source, 0), axis=0) * ALIGN).reshape(-1)

        done = []

        def in_turn(kernel, small, *args, follows=True):
            if done and follows:
                small = after(small, done[-1]) if done[-1].ndim else small + done[-1]
            out = kernel(small, *args)
            done.append(out[0] if isinstance(out, (list, tuple)) else out)
            return out

        wide_spans = list(spans(WIDE_CHUNKS))
        parts = [jnp.stack([w[0, :, : wide_spans[0][1]] for w in (wg_loc, wu_loc)])]
        later = after((wg_loc, wu_loc), parts[0])
        parts += [jnp.stack([w[l, :, lo : lo + n] for w in later]) for l in locals_ for lo, n in wide_spans if l or lo]
        parts += [wd_loc[l, :, lo : lo + n] for l, lo, n in DOWN_PIECES]
        far = []

        def cross():
            if len(far) == len(parts):
                return
            piece = parts[len(far)]
            if len(far) >= 2:
                piece = after(piece, far[-2])
            far.append(lax.ppermute(piece, "data", swap))

        def exchange(blocks, step):
            out = [blocks[0]]
            for d in range(1, n_group):
                out.append(lax.ppermute(blocks[d], "expert", [(s, (s + step * d) % n_group) for s in range(n_group)]))
            return out

        def mix(y_loc, col, width, back):
            col = col.astype(I32)[None]
            back = [(back[l][0][d], back[l][1]) for d in range(n_group) for l in locals_]
            out = in_turn(mix_cols, col, y_loc, x_loc, pos, gate_loc, chunks, width, back)
            done[-1] = out[1][0]
            return out[0]

        cross()
        cross()
        first_blk = after(first_blk, meta)
        rows = [exchange(in_turn(pack_rows, first_blk, x_loc, slot_te, n_exp, n_local, 0, capacity), 1)]
        cross()
        packed = in_turn(pack_rows, first_blk, x_loc, slot_te, n_exp, n_local, 1, capacity)
        cross()
        rows.append(exchange([after(block, rows[0]) for block in packed], 1))

        n_wide = len(wide_spans)
        hidden, own = [], []
        for l in locals_:
            hidden.append(None)
            for k, (lo, n) in enumerate(wide_spans):
                if l or k >= 2:
                    cross()
                hidden[l] = in_turn(wide_part, meta[l], hidden[l], rows[l], wg_loc, wu_loc, far[l * n_wide + k], l, lo, n, follows=k == 0)
            own.append(exchange(in_turn(down_part, meta[l], hidden[l], wd_loc, n_group, l, follows=False), -1))

        def far_piece(i):
            cross()
            l = DOWN_PIECES[i][0]
            return exchange(in_turn(down_part, meta[l], hidden[l], far[n_local * n_wide + i], n_group), -1)

        far_col = (1 - side) * half
        ret = [far_piece(0), far_piece(1)]
        y_loc = mix(None, side * half, half, [(own[l], 0) for l in locals_])
        ret += [far_piece(2), far_piece(3)]
        y_loc = mix(y_loc, far_col, 512, [(ret[0], 0), (ret[1], 0)])
        ret += [far_piece(4), far_piece(5), far_piece(6)]
        y_loc = mix(y_loc, far_col + 512, 256, [(ret[2], 0), (ret[3], 0)])
        y_loc = mix(y_loc, far_col + 768, 128, [(ret[4], 0), (ret[5], 0)])
        return mix(y_loc, far_col + 896, 128, [(ret[4], 1), (ret[6], 0)])

    in_specs = (tok_spec, tok_spec, tok_spec, wide_spec, wide_spec, down_spec)
    return jax.shard_map(whole_step, mesh=mesh, in_specs=in_specs, out_specs=tok_spec, check_vma=False)
```

```python
import functools

import jax
import jax.numpy as jnp
from jax import lax
from jax.experimental import pallas as pl
from jax.experimental.pallas import tpu as pltpu
from jax.sharding import PartitionSpec as P


BF16 = jnp.bfloat16
F32 = jnp.float32
I32 = jnp.int32
VMEM_LIMIT = 66_000_000

TILE = 256
TOK_BLOCK = 256
MIX_TILE = 128
MIX_UNROLL = 4
ALIGN = 16
REACH = 512
DEEP = 4
DOWN_BLOCK = 512
SUB = 512
WIDE_CHUNKS = (512, 2048, 1536, 1536)
DOWN_PIECES = (
    (0, 0, 512, (0, 11)),
    (1, 0, 512, (0, 11)),
    (0, 512, 256, (0, 11)),
    (1, 512, 256, (0, 11)),
    (0, 768, 256, (0, 11)),
    (1, 768, 128, (0, 11)),
    (1, 896, 128, (0, 8)),
    (1, 896, 128, (8, 11)),
)
DOWN_SHARES = 11


def capacity_rows(tok_rows, top_k, n_exp):
    return max(8, ((5 * top_k * tok_rows) // (4 * n_exp) + 7) // 8 * 8)


def after(value, *earlier):
    return lax.optimization_barrier((value, earlier))[0]


def any_spec():
    return pl.BlockSpec(memory_space=pl.ANY)


def pack_body(n_local, local, n_blk, n_group, first_ref, slot_ref, x_ref, *refs):
    out_refs, acc_ref = refs[:n_group], refs[n_group]
    e, s = pl.program_id(0) * n_local + local, pl.program_id(1)
    count = first_ref[e * (n_blk + 1) + n_blk]
    base = s * TILE

    @pl.when(base < count)
    def _():
        end = jnp.minimum(base + TILE, count)
        lo = jnp.int32(0)
        hi = jnp.int32(0)
        for i in range(n_blk):
            lo += (first_ref[e * (n_blk + 1) + i + 1] <= base).astype(I32)
            hi += (first_ref[e * (n_blk + 1) + i] < end).astype(I32)
        acc_ref[...] = jnp.zeros_like(acc_ref)
        slots = base + lax.broadcasted_iota(I32, (TILE, TOK_BLOCK), 0)

        def visit(i, carry):
            off = pl.multiple_of(i * TOK_BLOCK, TOK_BLOCK)
            pick = (slots == slot_ref[pl.ds(e, 1), pl.ds(off, TOK_BLOCK)]).astype(F32).astype(BF16)
            acc_ref[...] += jnp.dot(pick, x_ref[pl.ds(off, TOK_BLOCK), :], preferred_element_type=F32)
            return carry

        lax.fori_loop(lo, hi, visit, 0)
        for d in range(n_group):

            @pl.when(pl.program_id(0) == d)
            def _():
                out_refs[d][...] = acc_ref[...].astype(BF16)


def pack_rows(first_blk, x_loc, slot_te, n_exp, n_local, local, capacity):
    tok_rows, d_model = x_loc.shape
    n_blk = tok_rows // TOK_BLOCK
    n_group = n_exp // n_local

    def out_spec(d):
        def index(p, s, first):
            used = (first[(d * n_local + local) * (n_blk + 1) + n_blk] + TILE - 1) // TILE
            last = jnp.maximum(used - 1, 0)
            return jnp.where(p < d, 0, jnp.where(p > d, last, jnp.minimum(s, last))), 0

        return pl.BlockSpec((TILE, d_model), index)

    return pl.pallas_call(
        functools.partial(pack_body, n_local, local, n_blk, n_group),
        grid_spec=pltpu.PrefetchScalarGridSpec(
            num_scalar_prefetch=1,
            grid=(n_group, capacity // TILE),
            in_specs=[
                pl.BlockSpec((n_exp, tok_rows), lambda p, s, f: (0, 0)),
                pl.BlockSpec((tok_rows, d_model), lambda p, s, f: (0, 0)),
            ],
            out_specs=[out_spec(d) for d in range(n_group)],
            scratch_shapes=[pltpu.VMEM((TILE, d_model), F32)],
        ),
        out_shape=[jax.ShapeDtypeStruct((capacity, d_model), BF16)] * n_group,
        compiler_params=pltpu.CompilerParams(vmem_limit_bytes=VMEM_LIMIT),
        cost_estimate=pl.CostEstimate(flops=20_000_000_000, bytes_accessed=60_000_000, transcendentals=0),
        name="pack_rows",
    )(first_blk, slot_te, x_loc)


def smem():
    return pl.BlockSpec(memory_space=pltpu.SMEM)


def tile_at(i):
    return pl.ds(pl.multiple_of(i * TILE, TILE), TILE)


def wide_body(n_group, local, lo_col, cols, meta_ref, *refs):
    x_refs = refs[:n_group]
    wg_ref, wu_ref, far_ref = refs[n_group : n_group + 3]
    h_ref, rows_buf, h_buf, gate_w, up_w, row_sems, h_sems, sems = refs[-8:]
    side = meta_ref[0]
    half = wg_ref.shape[1]
    n_live = meta_ref[1 + n_group]

    def fetch(i):
        for d in range(n_group):

            @pl.when((i >= meta_ref[1 + d]) & (i < meta_ref[2 + d]))
            def _():
                pltpu.make_async_copy(x_refs[d].at[tile_at(i - meta_ref[1 + d]), :], rows_buf.at[i % 2], row_sems.at[i % 2]).start()

    def send(i):
        return pltpu.make_async_copy(h_buf.at[i % 2], h_ref.at[tile_at(i), pl.ds(lo_col, cols)], h_sems.at[i % 2])

    fetch(0)
    near = pl.ds(pl.multiple_of(side * half, half), half)
    far = pl.ds(pl.multiple_of((1 - side) * half, half), half)
    copies = [
        pltpu.make_async_copy(wg_ref.at[local, :, pl.ds(lo_col, cols)], gate_w.at[near, :], sems.at[0]),
        pltpu.make_async_copy(wu_ref.at[local, :, pl.ds(lo_col, cols)], up_w.at[near, :], sems.at[1]),
        pltpu.make_async_copy(far_ref.at[0], gate_w.at[far, :], sems.at[2]),
        pltpu.make_async_copy(far_ref.at[1], up_w.at[far, :], sems.at[3]),
    ]
    for copy in copies:
        copy.start()
    for copy in copies:
        copy.wait()

    def step(i, carry):
        fetch(i + 1)
        pltpu.make_async_copy(x_refs[0].at[tile_at(0), :], rows_buf.at[i % 2], row_sems.at[i % 2]).wait()

        @pl.when(i >= 2)
        def _():
            send(i - 2).wait()

        def part(j, carry):
            span = pl.ds(pl.multiple_of(j * SUB, SUB), SUB)
            rows = rows_buf[i % 2]
            g = jnp.dot(rows, gate_w[:, span], preferred_element_type=F32)
            u = jnp.dot(rows, up_w[:, span], preferred_element_type=F32)
            h_buf[i % 2, :, span] = (jax.nn.silu(g) * u).astype(BF16)
            return carry

        lax.fori_loop(0, cols // SUB, part, 0)
        send(i).start()
        return carry

    lax.fori_loop(0, n_live, step, 0)
    for back in (2, 1):

        @pl.when(n_live >= back)
        def _():
            send(n_live - back).wait()


def wide_part(meta, hidden, rows, w_gate, w_up, far, local, lo_col, cols):
    n_group = len(rows)
    capacity, d_model = rows[0].shape
    n_rows = n_group * capacity
    ffn = w_gate.shape[2]
    args = [meta, *rows, w_gate, w_up, far]
    alias = {}
    if hidden is not None:
        alias = {len(args): 0}
        args.append(hidden)
    return pl.pallas_call(
        functools.partial(wide_body, n_group, local, lo_col, cols),
        in_specs=[smem()] + [any_spec()] * (len(args) - 1),
        out_specs=any_spec(),
        scratch_shapes=[
            pltpu.VMEM((2, TILE, d_model), BF16),
            pltpu.VMEM((2, TILE, cols), BF16),
            pltpu.VMEM((d_model, cols), BF16),
            pltpu.VMEM((d_model, cols), BF16),
            pltpu.SemaphoreType.DMA((2,)),
            pltpu.SemaphoreType.DMA((2,)),
            pltpu.SemaphoreType.DMA((4,)),
        ],
        out_shape=jax.ShapeDtypeStruct((n_rows, ffn), BF16),
        input_output_aliases=alias,
        compiler_params=pltpu.CompilerParams(vmem_limit_bytes=VMEM_LIMIT),
        cost_estimate=pl.CostEstimate(flops=4 * n_rows * d_model * cols, bytes_accessed=n_rows * d_model * 2, transcendentals=0),
        name="wide_part",
    )(*args)


def down_body(n_group, local, lo_hid, adds, partial, meta_ref, h_ref, w_ref, *refs):
    sum_ref, refs = (refs[0], refs[1:]) if adds else (None, refs)
    n_out = 1 if partial else n_group
    out_refs = refs[:n_out]
    h_buf, out_buf, w_buf, sum_buf, h_sems, out_sems, sum_sems, sem = refs[n_out:]
    n_live = meta_ref[1 + n_group]
    hid = pl.ds(lo_hid, w_buf.shape[0])
    block = min(w_buf.shape[1], DOWN_BLOCK)

    def fetches(i):
        copies = [pltpu.make_async_copy(h_ref.at[tile_at(i), hid], h_buf.at[i % DEEP], h_sems.at[i % DEEP])]
        if adds:
            copies.append(pltpu.make_async_copy(sum_ref.at[tile_at(i), :], sum_buf.at[i % DEEP], sum_sems.at[i % DEEP]))
        return copies

    def sent(i):
        pltpu.make_async_copy(out_buf.at[i % 2], out_refs[0].at[tile_at(0), :], out_sems.at[i % 2]).wait()

    def send(i, there, tile):
        pltpu.make_async_copy(out_buf.at[i % 2], there.at[tile_at(tile), :], out_sems.at[i % 2]).start()

    for i in range(DEEP - 1):

        @pl.when(i < n_live)
        def _():
            for copy in fetches(i):
                copy.start()

    copy = pltpu.make_async_copy(w_ref if local is None else w_ref.at[local], w_buf, sem)
    copy.start()
    copy.wait()

    def step(i, carry):
        @pl.when(i + DEEP - 1 < n_live)
        def _():
            for copy in fetches(i + DEEP - 1):
                copy.start()

        for copy in fetches(i):
            copy.wait()

        @pl.when(i >= 2)
        def _():
            sent(i)

        def part(j, carry):
            span = pl.ds(pl.multiple_of(j * block, block), block)
            total = jnp.dot(h_buf[i % DEEP], w_buf[:, span], preferred_element_type=F32)
            if adds:
                total += sum_buf[i % DEEP, :, span]
            out_buf[i % 2, :, span] = total.astype(out_buf.dtype)
            return carry

        lax.fori_loop(0, w_buf.shape[1] // block, part, 0)
        if partial:
            send(i, out_refs[0], i)
            return carry
        for d in range(n_group):

            @pl.when((i >= meta_ref[1 + d]) & (i < meta_ref[2 + d]))
            def _():
                send(i, out_refs[d], i - meta_ref[1 + d])

        return carry

    lax.fori_loop(0, n_live, step, 0)
    for back in (2, 1):

        @pl.when(n_live >= back)
        def _():
            sent(n_live - back)

    for d in range(0 if partial else n_group):
        @pl.when(meta_ref[1 + d] == meta_ref[2 + d])
        def _():
            out_buf[0] = jnp.zeros_like(out_buf[0])
            send(0, out_refs[d], 0)
            sent(0)


def down_part(meta, hidden, weight, n_group, local=None, lo_hid=0, sums=None, partial=False):
    n_rows = hidden.shape[0]
    n_hid, width = weight.shape[-2:]
    adds = sums is not None
    out_type = F32 if partial else BF16
    rows = n_rows if partial else n_rows // n_group
    return pl.pallas_call(
        functools.partial(down_body, n_group, local, lo_hid, adds, partial),
        in_specs=[smem()] + [any_spec()] * (2 + adds),
        out_specs=[any_spec()] * (1 if partial else n_group),
        scratch_shapes=[
            pltpu.VMEM((DEEP, TILE, n_hid), BF16),
            pltpu.VMEM((2, TILE, width), out_type),
            pltpu.VMEM((n_hid, width), BF16),
            pltpu.VMEM((DEEP, TILE, width) if adds else (DEEP, 8, 128), F32),
            pltpu.SemaphoreType.DMA((DEEP,)),
            pltpu.SemaphoreType.DMA((2,)),
            pltpu.SemaphoreType.DMA((DEEP,)),
            pltpu.SemaphoreType.DMA,
        ],
        out_shape=[jax.ShapeDtypeStruct((rows, width), out_type)] * (1 if partial else n_group),
        compiler_params=pltpu.CompilerParams(vmem_limit_bytes=VMEM_LIMIT),
        cost_estimate=pl.CostEstimate(flops=2 * n_rows * n_hid * width, bytes_accessed=n_rows * n_hid * 2, transcendentals=0),
        name="down_part",
    )(meta, hidden, weight, *([sums] if adds else []))


def mix_body(n_exp, n_tile, subs, widths, col_ref, chunk_ref, pos_ref, gate_ref, x_ref, *refs):
    n_set = len(widths)
    back_refs = refs[: n_set * n_exp]
    y_ref, mark_ref = refs[-3 - 4 * n_set : -1 - 4 * n_set]
    bufs, sems = refs[-1 - 4 * n_set : -1], refs[-1]
    sets, copies = [], []
    for g, width in enumerate(widths):
        back_buf, near_buf, x_buf, y_buf = bufs[4 * g : 4 * g + 4]
        cols = pl.ds(pl.multiple_of(col_ref[g], 128), width)
        sets.append((back_buf, near_buf, x_buf, y_buf, cols))
        for e in range(n_exp):
            ref, sub = back_refs[g * n_exp + e], subs[g * n_exp + e]
            capacity = ref.shape[0]
            here = back_buf.at[pl.ds(e * capacity, capacity), :]
            copies.append(pltpu.make_async_copy(ref.at[:, pl.ds(sub * width, width)], here, sems.at[len(copies)]))
        copies.append(pltpu.make_async_copy(x_ref.at[:, cols], x_buf, sems.at[len(copies)]))
    for copy in copies:
        copy.start()
    for copy in copies:
        copy.wait()

    def step(block, carry):
        for k in range(MIX_UNROLL):
            i = block * MIX_UNROLL + k
            tokens = pl.ds(pl.multiple_of(i * MIX_TILE, MIX_TILE), MIX_TILE)
            seat = lax.broadcasted_iota(I32, (MIX_TILE, REACH), 1)
            pick = jnp.concatenate([(seat == pos_ref[tokens, j : j + 1]).astype(F32).astype(BF16) for j in range(2)], axis=0)
            for back_buf, near_buf, x_buf, y_buf, _ in sets:
                for c in range(REACH // ALIGN):
                    chunk = pl.multiple_of(chunk_ref[i * (REACH // ALIGN) + c], ALIGN)
                    near_buf[k, c * ALIGN : (c + 1) * ALIGN, :] = back_buf[pl.ds(chunk, ALIGN), :]
                found = jnp.dot(pick, near_buf[k], preferred_element_type=F32)
                mixed = gate_ref[tokens, 0:1] * found[:MIX_TILE] + gate_ref[tokens, 1:2] * found[MIX_TILE:]
                y_buf[tokens, :] = (x_buf[tokens, :].astype(F32) + mixed).astype(BF16)
        return carry

    lax.fori_loop(0, n_tile // MIX_UNROLL, step, 0)
    outs = [pltpu.make_async_copy(y_buf, y_ref.at[:, cols], sems.at[g]) for g, (_, _, _, y_buf, cols) in enumerate(sets)]
    for out in outs:
        out.start()
    for out in outs:
        out.wait()
    mark_ref[0] = 0


def mix_cols(col, y_loc, x_loc, pos, gate_loc, chunks, widths, back):
    tok_rows, d_model = x_loc.shape
    n_exp = len(back) // len(widths)
    capacity = back[0][0].shape[0]
    vmem = pl.BlockSpec(memory_space=pltpu.VMEM)
    args = [col, chunks, pos, gate_loc, x_loc, *[array for array, _ in back]]
    specs = [smem(), smem(), vmem, vmem, any_spec()] + [any_spec()] * len(back)
    alias = {}
    if y_loc is not None:
        alias = {len(args): 0}
        args.append(y_loc)
        specs.append(any_spec())
    bufs = []
    for width in widths:
        bufs += [
            pltpu.VMEM((n_exp * capacity, width), BF16),
            pltpu.VMEM((MIX_UNROLL, REACH, width), BF16),
            pltpu.VMEM((tok_rows, width), BF16),
            pltpu.VMEM((tok_rows, width), BF16),
        ]
    return pl.pallas_call(
        functools.partial(mix_body, n_exp, tok_rows // MIX_TILE, tuple(sub for _, sub in back), widths),
        in_specs=specs,
        out_specs=[any_spec(), smem()],
        scratch_shapes=bufs + [pltpu.SemaphoreType.DMA(((n_exp + 1) * len(widths),))],
        out_shape=[jax.ShapeDtypeStruct((tok_rows, d_model), BF16), jax.ShapeDtypeStruct((1,), I32)],
        input_output_aliases=alias,
        compiler_params=pltpu.CompilerParams(vmem_limit_bytes=VMEM_LIMIT),
        cost_estimate=pl.CostEstimate(flops=20_000_000 * sum(widths), bytes_accessed=20_000 * sum(widths), transcendentals=0),
        name="mix_cols",
    )(*args)


def spans(sizes):
    lo = 0
    for size in sizes:
        yield lo, size
        lo += size


def solution(mesh):
    n_group, n_side = mesh.shape["expert"], mesh.shape["data"]
    tok_spec = P(("rep", "expert", "data"), None)
    wide_spec = P("expert", "data", None)
    down_spec = P("expert", None, "data")
    swap = [(s, 1 - s) for s in range(n_side)]

    def whole_step(x_loc, idx_loc, gate_loc, wg_loc, wu_loc, wd_loc):
        tok_rows, _ = x_loc.shape
        top_k = idx_loc.shape[1]
        n_local, half, ffn = wg_loc.shape
        n_exp = n_local * n_group
        capacity = capacity_rows(tok_rows, top_k, n_exp)
        side = lax.axis_index("data")
        place = lax.axis_index("expert")
        locals_ = range(n_local)
        groups = jnp.arange(n_group, dtype=I32)

        ids = ((idx_loc // n_local + n_group - place) % n_group * n_local + idx_loc % n_local).T
        experts = jnp.arange(n_exp, dtype=I32)[:, None]
        chosen = functools.reduce(jnp.logical_or, [ids[j][None, :] == experts for j in range(top_k)])
        chosen_i = chosen.astype(I32)
        running = jnp.cumsum(chosen_i, axis=1)
        before = running - chosen_i
        slot_te = jnp.where(chosen & (before < capacity), before, -1)
        counts = jnp.minimum(running[:, -1], capacity)
        first = jnp.minimum(before, capacity)
        first_blk = jnp.concatenate([first[:, ::TOK_BLOCK], counts[:, None]], axis=1).reshape(-1)
        first_mix = first[:, ::MIX_TILE]

        table = lax.all_gather(counts, "expert")
        meta = []
        for l in locals_:
            mine = jnp.sum(jnp.where(((place - groups) % n_group)[:, None, None] == groups[None, :, None], table.reshape(n_group, n_group, n_local)[None, :, :, l] * (groups[:, None, None] == groups[None, None, :]), 0), axis=(1, 2))
            ends = jnp.cumsum((mine + TILE - 1) // TILE)
            meta.append(jnp.concatenate([side[None], jnp.zeros((1,), I32), ends]).astype(I32))

        reach = REACH // ALIGN
        start = first_mix // ALIGN
        stop = jnp.concatenate([first_mix[:, 1:], counts[:, None]], axis=1)
        size = jnp.where(stop > first_mix, (stop + ALIGN - 1) // ALIGN - start, 0)
        lead = jnp.cumsum(size, axis=0) - size
        at = slot_te + jnp.repeat((lead - start) * ALIGN, MIX_TILE, axis=1)
        at = jnp.where(slot_te < 0, -1, at)
        pos = jnp.stack([jnp.sum(jnp.where(ids[j][None, :] == experts, at, 0), axis=0) for j in range(top_k)], axis=1)
        seat = jnp.arange(reach, dtype=I32)[None, None, :]
        taken = (seat >= lead[:, :, None]) & (seat < (lead + size)[:, :, None])
        source = experts[:, :, None] * (capacity // ALIGN) + (start - lead)[:, :, None] + seat
        chunks = (jnp.sum(jnp.where(taken, source, 0), axis=0) * ALIGN).reshape(-1)

        done = []

        def in_turn(kernel, small, *args, follows=True):
            if done and follows:
                small = after(small, done[-1]) if done[-1].ndim else small + done[-1]
            out = kernel(small, *args)
            done.append(out[0] if isinstance(out, (list, tuple)) else out)
            return out

        wide_spans = list(spans(WIDE_CHUNKS))
        parts = [jnp.stack([w[0, :, : wide_spans[0][1]] for w in (wg_loc, wu_loc)])]
        later = after((wg_loc, wu_loc), parts[0])
        parts += [jnp.stack([w[l, :, lo : lo + n] for w in later]) for l in locals_ for lo, n in wide_spans if l or lo]
        hid = [(first * ffn // DOWN_SHARES, stop * ffn // DOWN_SHARES) for *_, (first, stop) in DOWN_PIECES]
        parts += [wd_loc[l, a:b, lo : lo + n] for (l, lo, n, _), (a, b) in zip(DOWN_PIECES, hid)]
        far = []

        def cross():
            if len(far) == len(parts):
                return
            piece = parts[len(far)]
            if len(far) >= 2:
                piece = after(piece, far[-2])
            far.append(lax.ppermute(piece, "data", swap))

        def exchange(blocks, step):
            out = [blocks[0]]
            for d in range(1, n_group):
                out.append(lax.ppermute(blocks[d], "expert", [(s, (s + step * d) % n_group) for s in range(n_group)]))
            return out

        def mix(y_loc, *sets):
            col = jnp.stack([col for col, _, _ in sets]).astype(I32)
            back = [(pair[l][0][d], pair[l][1]) for _, _, pair in sets for d in range(n_group) for l in locals_]
            out = in_turn(mix_cols, col, y_loc, x_loc, pos, gate_loc, chunks, tuple(width for _, width, _ in sets), back)
            done[-1] = out[1][0]
            return out[0]

        cross()
        cross()
        first_blk = after(first_blk, meta)
        rows = [exchange(in_turn(pack_rows, first_blk, x_loc, slot_te, n_exp, n_local, 0, capacity), 1)]
        cross()
        packed = in_turn(pack_rows, first_blk, x_loc, slot_te, n_exp, n_local, 1, capacity)
        cross()
        rows.append(exchange([after(block, rows[0]) for block in packed], 1))

        n_wide = len(wide_spans)
        hidden, own = [], []
        for l in locals_:
            hidden.append(None)
            for k, (lo, n) in enumerate(wide_spans):
                if k >= 2 or (l and k):
                    cross()
                hidden[l] = in_turn(wide_part, meta[l], hidden[l], rows[l], wg_loc, wu_loc, far[l * n_wide + k], l, lo, n, follows=k == 0)
            if l == 0:
                cross()
            own.append(exchange(in_turn(down_part, meta[l], hidden[l], wd_loc, n_group, l, follows=False), -1))

        def far_piece(i, sums=None, partial=False):
            cross()
            l = DOWN_PIECES[i][0]
            out = in_turn(down_part, meta[l], hidden[l], far[n_local * n_wide + i], n_group, None, hid[i][0], sums, partial)
            return out[0] if partial else exchange(out, -1)

        far_col = (1 - side) * half
        ret = [far_piece(0), far_piece(1)]
        y_loc = mix(None, (side * half, half, [(own[l], 0) for l in locals_]))
        ret += [far_piece(2), far_piece(3)]
        y_loc = mix(y_loc, (far_col, 512, [(ret[0], 0), (ret[1], 0)]))
        ret += [far_piece(4), far_piece(5)]
        ret.append(far_piece(7, far_piece(6, partial=True)))
        y_loc = mix(y_loc, (far_col + 512, 256, [(ret[2], 0), (ret[3], 0)]), (far_col + 768, 128, [(ret[4], 0), (ret[5], 0)]))
        return mix(y_loc, (far_col + 896, 128, [(ret[4], 1), (ret[6], 0)]))

    in_specs = (tok_spec, tok_spec, tok_spec, wide_spec, wide_spec, down_spec)
    return jax.shard_map(whole_step, mesh=mesh, in_specs=in_specs, out_specs=tok_spec, check_vma=False)
```

```python
import functools

import jax
import jax.numpy as jnp
from jax import lax
from jax.experimental import pallas as pl
from jax.experimental.pallas import tpu as pltpu
from jax.sharding import PartitionSpec as P


BF16 = jnp.bfloat16
F32 = jnp.float32
I32 = jnp.int32
VMEM_LIMIT = 66_000_000

TILE = 256
TOK_BLOCK = 256
MIX_TILE = 128
ALIGN = 16
REACH = 512
DOWN_BLOCK = 512
SUB = 512
WIDE_CHUNKS = (512, 2048, 1536, 1536)
DOWN_PIECES = (
    (0, 0, 512, (0, 11)),
    (1, 0, 512, (0, 11)),
    (0, 512, 256, (0, 11)),
    (1, 512, 256, (0, 11)),
    (0, 768, 256, (0, 11)),
    (1, 768, 128, (0, 11)),
    (1, 896, 128, (0, 8)),
    (1, 896, 128, (8, 11)),
)
DOWN_SHARES = 11


def capacity_rows(tok_rows, top_k, n_exp):
    return max(8, ((5 * top_k * tok_rows) // (4 * n_exp) + 7) // 8 * 8)


def after(value, *earlier):
    return lax.optimization_barrier((value, earlier))[0]


def any_spec():
    return pl.BlockSpec(memory_space=pl.ANY)


def pack_body(n_local, local, n_blk, n_group, first_ref, slot_ref, x_ref, *refs):
    out_refs, acc_ref = refs[:n_group], refs[n_group]
    e, s = pl.program_id(0) * n_local + local, pl.program_id(1)
    count = first_ref[e * (n_blk + 1) + n_blk]
    base = s * TILE

    @pl.when(base < count)
    def _():
        end = jnp.minimum(base + TILE, count)
        lo = jnp.int32(0)
        hi = jnp.int32(0)
        for i in range(n_blk):
            lo += (first_ref[e * (n_blk + 1) + i + 1] <= base).astype(I32)
            hi += (first_ref[e * (n_blk + 1) + i] < end).astype(I32)
        acc_ref[...] = jnp.zeros_like(acc_ref)
        slots = base + lax.broadcasted_iota(I32, (TILE, TOK_BLOCK), 0)

        def visit(i, carry):
            off = pl.multiple_of(i * TOK_BLOCK, TOK_BLOCK)
            pick = (slots == slot_ref[pl.ds(e, 1), pl.ds(off, TOK_BLOCK)]).astype(F32).astype(BF16)
            acc_ref[...] += jnp.dot(pick, x_ref[pl.ds(off, TOK_BLOCK), :], preferred_element_type=F32)
            return carry

        lax.fori_loop(lo, hi, visit, 0)
        for d in range(n_group):

            @pl.when(pl.program_id(0) == d)
            def _():
                out_refs[d][...] = acc_ref[...].astype(BF16)


def pack_rows(first_blk, x_loc, slot_te, n_exp, n_local, local, capacity):
    tok_rows, d_model = x_loc.shape
    n_blk = tok_rows // TOK_BLOCK
    n_group = n_exp // n_local

    def out_spec(d):
        def index(p, s, first):
            used = (first[(d * n_local + local) * (n_blk + 1) + n_blk] + TILE - 1) // TILE
            last = jnp.maximum(used - 1, 0)
            return jnp.where(p < d, 0, jnp.where(p > d, last, jnp.minimum(s, last))), 0

        return pl.BlockSpec((TILE, d_model), index)

    return pl.pallas_call(
        functools.partial(pack_body, n_local, local, n_blk, n_group),
        grid_spec=pltpu.PrefetchScalarGridSpec(
            num_scalar_prefetch=1,
            grid=(n_group, capacity // TILE),
            in_specs=[
                pl.BlockSpec((n_exp, tok_rows), lambda p, s, f: (0, 0)),
                pl.BlockSpec((tok_rows, d_model), lambda p, s, f: (0, 0)),
            ],
            out_specs=[out_spec(d) for d in range(n_group)],
            scratch_shapes=[pltpu.VMEM((TILE, d_model), F32)],
        ),
        out_shape=[jax.ShapeDtypeStruct((capacity, d_model), BF16)] * n_group,
        compiler_params=pltpu.CompilerParams(vmem_limit_bytes=VMEM_LIMIT),
        cost_estimate=pl.CostEstimate(flops=20_000_000_000, bytes_accessed=60_000_000, transcendentals=0),
        name="pack_rows",
    )(first_blk, slot_te, x_loc)


def smem():
    return pl.BlockSpec(memory_space=pltpu.SMEM)


def tile_at(i):
    return pl.ds(pl.multiple_of(i * TILE, TILE), TILE)


def wide_body(n_group, local, lo_col, cols, meta_ref, *refs):
    x_refs = refs[:n_group]
    wg_ref, wu_ref, far_ref = refs[n_group : n_group + 3]
    h_ref, rows_buf, h_buf, gate_w, up_w, row_sems, h_sems, sems = refs[-8:]
    side = meta_ref[0]
    half = wg_ref.shape[1]
    n_live = meta_ref[1 + n_group]

    def fetch(i):
        for d in range(n_group):

            @pl.when((i >= meta_ref[1 + d]) & (i < meta_ref[2 + d]))
            def _():
                pltpu.make_async_copy(x_refs[d].at[tile_at(i - meta_ref[1 + d]), :], rows_buf.at[i % 2], row_sems.at[i % 2]).start()

    def send(i):
        return pltpu.make_async_copy(h_buf.at[i % 2], h_ref.at[tile_at(i), pl.ds(lo_col, cols)], h_sems.at[i % 2])

    fetch(0)
    near = pl.ds(pl.multiple_of(side * half, half), half)
    far = pl.ds(pl.multiple_of((1 - side) * half, half), half)
    copies = [
        pltpu.make_async_copy(wg_ref.at[local, :, pl.ds(lo_col, cols)], gate_w.at[near, :], sems.at[0]),
        pltpu.make_async_copy(wu_ref.at[local, :, pl.ds(lo_col, cols)], up_w.at[near, :], sems.at[1]),
        pltpu.make_async_copy(far_ref.at[0], gate_w.at[far, :], sems.at[2]),
        pltpu.make_async_copy(far_ref.at[1], up_w.at[far, :], sems.at[3]),
    ]
    for copy in copies:
        copy.start()
    for copy in copies:
        copy.wait()

    def step(i, carry):
        fetch(i + 1)
        pltpu.make_async_copy(x_refs[0].at[tile_at(0), :], rows_buf.at[i % 2], row_sems.at[i % 2]).wait()

        @pl.when(i >= 2)
        def _():
            send(i - 2).wait()

        def part(j, carry):
            span = pl.ds(pl.multiple_of(j * SUB, SUB), SUB)
            rows = rows_buf[i % 2]
            g = jnp.dot(rows, gate_w[:, span], preferred_element_type=F32)
            u = jnp.dot(rows, up_w[:, span], preferred_element_type=F32)
            h_buf[i % 2, :, span] = (jax.nn.silu(g) * u).astype(BF16)
            return carry

        lax.fori_loop(0, cols // SUB, part, 0)
        send(i).start()
        return carry

    lax.fori_loop(0, n_live, step, 0)
    for back in (2, 1):

        @pl.when(n_live >= back)
        def _():
            send(n_live - back).wait()


def wide_part(meta, hidden, rows, w_gate, w_up, far, local, lo_col, cols):
    n_group = len(rows)
    capacity, d_model = rows[0].shape
    n_rows = n_group * capacity
    ffn = w_gate.shape[2]
    args = [meta, *rows, w_gate, w_up, far]
    alias = {}
    if hidden is not None:
        alias = {len(args): 0}
        args.append(hidden)
    return pl.pallas_call(
        functools.partial(wide_body, n_group, local, lo_col, cols),
        in_specs=[smem()] + [any_spec()] * (len(args) - 1),
        out_specs=any_spec(),
        scratch_shapes=[
            pltpu.VMEM((2, TILE, d_model), BF16),
            pltpu.VMEM((2, TILE, cols), BF16),
            pltpu.VMEM((d_model, cols), BF16),
            pltpu.VMEM((d_model, cols), BF16),
            pltpu.SemaphoreType.DMA((2,)),
            pltpu.SemaphoreType.DMA((2,)),
            pltpu.SemaphoreType.DMA((4,)),
        ],
        out_shape=jax.ShapeDtypeStruct((n_rows, ffn), BF16),
        input_output_aliases=alias,
        compiler_params=pltpu.CompilerParams(vmem_limit_bytes=VMEM_LIMIT),
        cost_estimate=pl.CostEstimate(flops=4 * n_rows * d_model * cols, bytes_accessed=n_rows * d_model * 2, transcendentals=0),
        name="wide_part",
    )(*args)


def down_body(n_group, local, lo_hid, adds, partial, deep, pair_size, meta_ref, h_ref, w_ref, *refs):
    sum_ref, refs = (refs[0], refs[1:]) if adds else (None, refs)
    n_out = 1 if partial else n_group
    out_refs = refs[:n_out]
    h_buf, out_buf, w_buf, sum_buf, h_sems, out_sems, sum_sems, sem = refs[n_out:]
    n_live = meta_ref[1 + n_group]
    hid = pl.ds(lo_hid, w_buf.shape[0])
    block = min(w_buf.shape[1], DOWN_BLOCK)

    def fetches(i):
        copies = [pltpu.make_async_copy(h_ref.at[tile_at(i), hid], h_buf.at[i % deep], h_sems.at[i % deep])]
        if adds:
            copies.append(pltpu.make_async_copy(sum_ref.at[tile_at(i), :], sum_buf.at[i % deep], sum_sems.at[i % deep]))
        return copies

    def sent(i):
        pltpu.make_async_copy(out_buf.at[i % deep], out_refs[0].at[tile_at(0), :], out_sems.at[i % deep]).wait()

    def send(i, there, tile):
        pltpu.make_async_copy(out_buf.at[i % deep], there.at[tile_at(tile), :], out_sems.at[i % deep]).start()

    copy = pltpu.make_async_copy(w_ref if local is None else w_ref.at[local], w_buf, sem)
    copy.start()
    for i in range(deep - pair_size):

        @pl.when(i < n_live)
        def _():
            for fetch in fetches(i):
                fetch.start()

    copy.wait()

    def step(pair, carry):
        for k in range(pair_size):
            i = pair * pair_size + k

            @pl.when(i + deep - pair_size < n_live)
            def _():
                for fetch in fetches(i + deep - pair_size):
                    fetch.start()

        for k in range(pair_size):
            i = pair * pair_size + k

            @pl.when(i < n_live)
            def _():
                for fetch in fetches(i):
                    fetch.wait()

            @pl.when((i >= deep) & (i - deep < n_live))
            def _():
                sent(i)

        slots = pl.ds(pair % (deep // pair_size) * pair_size, pair_size)

        def part(j, carry):
            span = pl.ds(pl.multiple_of(j * block, block), block)
            total = jnp.dot(h_buf[slots].reshape(pair_size * TILE, -1), w_buf[:, span], preferred_element_type=F32)
            if adds:
                total += sum_buf[slots, :, span].reshape(pair_size * TILE, -1)
            out_buf[slots, :, span] = total.astype(out_buf.dtype).reshape(pair_size, TILE, -1)
            return carry

        lax.fori_loop(0, w_buf.shape[1] // block, part, 0)
        for k in range(pair_size):
            i = pair * pair_size + k
            if partial:

                @pl.when(i < n_live)
                def _():
                    send(i, out_refs[0], i)

                continue
            for d in range(n_group):

                @pl.when((i >= meta_ref[1 + d]) & (i < meta_ref[2 + d]))
                def _():
                    send(i, out_refs[d], i - meta_ref[1 + d])

        return carry

    n_pair = (n_live + pair_size - 1) // pair_size
    lax.fori_loop(0, n_pair, step, 0)
    for back in range(deep, 0, -1):
        i = n_pair * pair_size - back

        @pl.when((i >= 0) & (i < n_live))
        def _():
            sent(i)

    for d in range(0 if partial else n_group):
        @pl.when(meta_ref[1 + d] == meta_ref[2 + d])
        def _():
            out_buf[0] = jnp.zeros_like(out_buf[0])
            send(0, out_refs[d], 0)
            sent(0)


def down_part(meta, hidden, weight, n_group, local=None, lo_hid=0, sums=None, partial=False):
    n_rows = hidden.shape[0]
    n_hid, width = weight.shape[-2:]
    adds = sums is not None
    deep, pair_size = (6, 2) if width >= 512 else (4, 1)
    out_type = F32 if partial else BF16
    rows = n_rows if partial else n_rows // n_group
    return pl.pallas_call(
        functools.partial(down_body, n_group, local, lo_hid, adds, partial, deep, pair_size),
        in_specs=[smem()] + [any_spec()] * (2 + adds),
        out_specs=[any_spec()] * (1 if partial else n_group),
        scratch_shapes=[
            pltpu.VMEM((deep, TILE, n_hid), BF16),
            pltpu.VMEM((deep, TILE, width), out_type),
            pltpu.VMEM((n_hid, width), BF16),
            pltpu.VMEM((deep, TILE, width) if adds else (deep, 8, 128), F32),
            pltpu.SemaphoreType.DMA((deep,)),
            pltpu.SemaphoreType.DMA((deep,)),
            pltpu.SemaphoreType.DMA((deep,)),
            pltpu.SemaphoreType.DMA,
        ],
        out_shape=[jax.ShapeDtypeStruct((rows, width), out_type)] * (1 if partial else n_group),
        compiler_params=pltpu.CompilerParams(vmem_limit_bytes=VMEM_LIMIT),
        cost_estimate=pl.CostEstimate(flops=2 * n_rows * n_hid * width, bytes_accessed=n_rows * n_hid * 2, transcendentals=0),
        name="down_part",
    )(meta, hidden, weight, *([sums] if adds else []))


def mix_body(n_exp, n_tile, subs, widths, unroll, col_ref, chunk_ref, pos_ref, gate_ref, x_ref, *refs):
    n_set = len(widths)
    back_refs = refs[: n_set * n_exp]
    y_ref, mark_ref, pos_buf, gate_buf = refs[-6 - 4 * n_set : -2 - 4 * n_set]
    bufs, sems, y_sems = refs[-2 - 4 * n_set : -2], refs[-2], refs[-1]
    sets = []
    copies = [pltpu.make_async_copy(pos_ref, pos_buf, sems.at[0]), pltpu.make_async_copy(gate_ref, gate_buf, sems.at[1])]
    for g, width in enumerate(widths):
        back_buf, near_buf, x_buf, y_buf = bufs[4 * g : 4 * g + 4]
        cols = pl.ds(pl.multiple_of(col_ref[g], 128), width)
        sets.append((back_buf, near_buf, x_buf, y_buf, cols))
        for e in range(n_exp):
            ref, sub = back_refs[g * n_exp + e], subs[g * n_exp + e]
            capacity = ref.shape[0]
            here = back_buf.at[pl.ds(e * capacity, capacity), :]
            copies.append(pltpu.make_async_copy(ref.at[:, pl.ds(sub * width, width)], here, sems.at[len(copies)]))
        copies.append(pltpu.make_async_copy(x_ref.at[:, cols], x_buf, sems.at[len(copies)]))
    for copy in copies:
        copy.start()
    for copy in copies:
        copy.wait()

    def out(g, block):
        _, _, _, y_buf, cols = sets[g]
        rows = pl.ds(pl.multiple_of(block * (unroll * MIX_TILE), unroll * MIX_TILE), unroll * MIX_TILE)
        return pltpu.make_async_copy(y_buf.at[rows, :], y_ref.at[rows, cols], y_sems.at[g, block])

    def step(block, carry):
        for k in range(unroll):
            i = block * unroll + k
            tokens = pl.ds(pl.multiple_of(i * MIX_TILE, MIX_TILE), MIX_TILE)
            seat = lax.broadcasted_iota(I32, (MIX_TILE, REACH), 1)
            pick = jnp.concatenate([(seat == pos_buf[tokens, j : j + 1]).astype(F32).astype(BF16) for j in range(2)], axis=0)
            for back_buf, near_buf, x_buf, y_buf, _ in sets:
                for c in range(REACH // ALIGN):
                    chunk = pl.multiple_of(chunk_ref[i * (REACH // ALIGN) + c], ALIGN)
                    near_buf[k, c * ALIGN : (c + 1) * ALIGN, :] = back_buf[pl.ds(chunk, ALIGN), :]
                found = jnp.dot(pick, near_buf[k], preferred_element_type=F32)
                mixed = gate_buf[tokens, 0:1] * found[:MIX_TILE] + gate_buf[tokens, 1:2] * found[MIX_TILE:]
                y_buf[tokens, :] = (x_buf[tokens, :].astype(F32) + mixed).astype(BF16)
        for g in range(n_set):
            out(g, block).start()
        return carry

    lax.fori_loop(0, n_tile // unroll, step, 0)
    for block in range(n_tile // unroll):
        for g in range(n_set):
            out(g, block).wait()
    mark_ref[0] = 0


def mix_cols(col, y_loc, x_loc, pos, gate_loc, chunks, widths, back):
    tok_rows, d_model = x_loc.shape
    n_exp = len(back) // len(widths)
    capacity = back[0][0].shape[0]
    unroll = 4 if sum(widths) < 512 else 2
    args = [col, chunks, pos, gate_loc, x_loc, *[array for array, _ in back]]
    specs = [smem(), smem()] + [any_spec()] * (3 + len(back))
    alias = {}
    if y_loc is not None:
        alias = {len(args): 0}
        args.append(y_loc)
        specs.append(any_spec())
    bufs = [pltpu.VMEM(pos.shape, I32), pltpu.VMEM(gate_loc.shape, F32)]
    for width in widths:
        bufs += [
            pltpu.VMEM((n_exp * capacity, width), BF16),
            pltpu.VMEM((unroll, REACH, width), BF16),
            pltpu.VMEM((tok_rows, width), BF16),
            pltpu.VMEM((tok_rows, width), BF16),
        ]
    return pl.pallas_call(
        functools.partial(mix_body, n_exp, tok_rows // MIX_TILE, tuple(sub for _, sub in back), widths, unroll),
        in_specs=specs,
        out_specs=[any_spec(), smem()],
        scratch_shapes=bufs
        + [
            pltpu.SemaphoreType.DMA((2 + (n_exp + 1) * len(widths),)),
            pltpu.SemaphoreType.DMA((len(widths), tok_rows // MIX_TILE // unroll)),
        ],
        out_shape=[jax.ShapeDtypeStruct((tok_rows, d_model), BF16), jax.ShapeDtypeStruct((1,), I32)],
        input_output_aliases=alias,
        compiler_params=pltpu.CompilerParams(vmem_limit_bytes=VMEM_LIMIT),
        cost_estimate=pl.CostEstimate(flops=20_000_000 * sum(widths), bytes_accessed=20_000 * sum(widths), transcendentals=0),
        name="mix_cols",
    )(*args)


def spans(sizes):
    lo = 0
    for size in sizes:
        yield lo, size
        lo += size


def solution(mesh):
    n_group, n_side = mesh.shape["expert"], mesh.shape["data"]
    tok_spec = P(("rep", "expert", "data"), None)
    wide_spec = P("expert", "data", None)
    down_spec = P("expert", None, "data")
    swap = [(s, 1 - s) for s in range(n_side)]

    def whole_step(x_loc, idx_loc, gate_loc, wg_loc, wu_loc, wd_loc):
        tok_rows, _ = x_loc.shape
        top_k = idx_loc.shape[1]
        n_local, half, ffn = wg_loc.shape
        n_exp = n_local * n_group
        capacity = capacity_rows(tok_rows, top_k, n_exp)
        side = lax.axis_index("data")
        place = lax.axis_index("expert")
        locals_ = range(n_local)
        groups = jnp.arange(n_group, dtype=I32)

        ids = ((idx_loc // n_local + n_group - place) % n_group * n_local + idx_loc % n_local).T
        experts = jnp.arange(n_exp, dtype=I32)[:, None]
        chosen = functools.reduce(jnp.logical_or, [ids[j][None, :] == experts for j in range(top_k)])
        chosen_i = chosen.astype(I32)
        running = jnp.cumsum(chosen_i, axis=1)
        before = running - chosen_i
        slot_te = jnp.where(chosen & (before < capacity), before, -1)
        counts = jnp.minimum(running[:, -1], capacity)
        first = jnp.minimum(before, capacity)
        first_blk = jnp.concatenate([first[:, ::TOK_BLOCK], counts[:, None]], axis=1).reshape(-1)
        first_mix = first[:, ::MIX_TILE]

        table = lax.all_gather(counts, "expert")
        meta = []
        for l in locals_:
            mine = jnp.sum(jnp.where(((place - groups) % n_group)[:, None, None] == groups[None, :, None], table.reshape(n_group, n_group, n_local)[None, :, :, l] * (groups[:, None, None] == groups[None, None, :]), 0), axis=(1, 2))
            ends = jnp.cumsum((mine + TILE - 1) // TILE)
            meta.append(jnp.concatenate([side[None], jnp.zeros((1,), I32), ends]).astype(I32))

        reach = REACH // ALIGN
        start = first_mix // ALIGN
        stop = jnp.concatenate([first_mix[:, 1:], counts[:, None]], axis=1)
        size = jnp.where(stop > first_mix, (stop + ALIGN - 1) // ALIGN - start, 0)
        lead = jnp.cumsum(size, axis=0) - size
        at = slot_te + jnp.repeat((lead - start) * ALIGN, MIX_TILE, axis=1)
        at = jnp.where(slot_te < 0, -1, at)
        pos = jnp.stack([jnp.sum(jnp.where(ids[j][None, :] == experts, at, 0), axis=0) for j in range(top_k)], axis=1)
        seat = jnp.arange(reach, dtype=I32)[None, None, :]
        taken = (seat >= lead[:, :, None]) & (seat < (lead + size)[:, :, None])
        source = experts[:, :, None] * (capacity // ALIGN) + (start - lead)[:, :, None] + seat
        chunks = (jnp.sum(jnp.where(taken, source, 0), axis=0) * ALIGN).reshape(-1)

        done = []

        def in_turn(kernel, small, *args, follows=True):
            if done and follows:
                small = after(small, done[-1]) if done[-1].ndim else small + done[-1]
            out = kernel(small, *args)
            done.append(out[0] if isinstance(out, (list, tuple)) else out)
            return out

        wide_spans = list(spans(WIDE_CHUNKS))
        parts = [jnp.stack([w[0, :, : wide_spans[0][1]] for w in (wg_loc, wu_loc)])]
        later = after((wg_loc, wu_loc), parts[0])
        parts += [jnp.stack([w[l, :, lo : lo + n] for w in later]) for l in locals_ for lo, n in wide_spans if l or lo]
        hid = [(first * ffn // DOWN_SHARES, stop * ffn // DOWN_SHARES) for *_, (first, stop) in DOWN_PIECES]
        parts += [wd_loc[l, a:b, lo : lo + n] for (l, lo, n, _), (a, b) in zip(DOWN_PIECES, hid)]
        far = []

        def cross():
            if len(far) == len(parts):
                return
            piece = parts[len(far)]
            if len(far) >= 2:
                piece = after(piece, far[-2])
            far.append(lax.ppermute(piece, "data", swap))

        def exchange(blocks, step):
            out = [blocks[0]]
            for d in range(1, n_group):
                out.append(lax.ppermute(blocks[d], "expert", [(s, (s + step * d) % n_group) for s in range(n_group)]))
            return out

        def mix(y_loc, *sets):
            col = jnp.stack([col for col, _, _ in sets]).astype(I32)
            back = [(pair[l][0][d], pair[l][1]) for _, _, pair in sets for d in range(n_group) for l in locals_]
            out = in_turn(mix_cols, col, y_loc, x_loc, pos, gate_loc, chunks, tuple(width for _, width, _ in sets), back)
            done[-1] = out[1][0]
            return out[0]

        cross()
        cross()
        first_blk = after(first_blk, meta)
        rows = [exchange(in_turn(pack_rows, first_blk, x_loc, slot_te, n_exp, n_local, 0, capacity), 1)]
        cross()
        packed = in_turn(pack_rows, first_blk, x_loc, slot_te, n_exp, n_local, 1, capacity)
        cross()
        rows.append(exchange([after(block, rows[0]) for block in packed], 1))

        n_wide = len(wide_spans)
        hidden, own = [], []
        for l in locals_:
            hidden.append(None)
            for k, (lo, n) in enumerate(wide_spans):
                if k >= 2 or (l and k):
                    cross()
                hidden[l] = in_turn(wide_part, meta[l], hidden[l], rows[l], wg_loc, wu_loc, far[l * n_wide + k], l, lo, n, follows=k == 0)
            if l == 0:
                cross()
            own.append(exchange(in_turn(down_part, meta[l], hidden[l], wd_loc, n_group, l, follows=False), -1))

        def far_piece(i, sums=None, partial=False):
            cross()
            l = DOWN_PIECES[i][0]
            out = in_turn(down_part, meta[l], hidden[l], far[n_local * n_wide + i], n_group, None, hid[i][0], sums, partial)
            return out[0] if partial else exchange(out, -1)

        far_col = (1 - side) * half
        ret = [far_piece(0), far_piece(1)]
        y_loc = mix(None, (side * half, half, [(own[l], 0) for l in locals_]))
        ret += [far_piece(2), far_piece(3)]
        y_loc = mix(y_loc, (far_col, 512, [(ret[0], 0), (ret[1], 0)]))
        ret += [far_piece(4), far_piece(5)]
        ret.append(far_piece(7, far_piece(6, partial=True)))
        y_loc = mix(y_loc, (far_col + 512, 256, [(ret[2], 0), (ret[3], 0)]), (far_col + 768, 128, [(ret[4], 0), (ret[5], 0)]))
        return mix(y_loc, (far_col + 896, 128, [(ret[4], 1), (ret[6], 0)]))

    in_specs = (tok_spec, tok_spec, tok_spec, wide_spec, wide_spec, down_spec)
    return jax.shard_map(whole_step, mesh=mesh, in_specs=in_specs, out_specs=tok_spec, check_vma=False)
```

```python
import functools

import jax
import jax.numpy as jnp
from jax import lax
from jax.experimental import pallas as pl
from jax.experimental.pallas import tpu as pltpu
from jax.sharding import PartitionSpec as P


BF16 = jnp.bfloat16
F32 = jnp.float32
I32 = jnp.int32
VMEM_LIMIT = 66_000_000

TILE = 256
TOK_BLOCK = 256
MIX_TILE = 128
ALIGN = 16
REACH = 512
DOWN_BLOCK = 512
SUB = 512
WIDE_CHUNKS = (512, 2048, 1536, 1536)
DOWN_PIECES = ((0, 0, 512), (1, 0, 512), (0, 512, 256), (1, 512, 256), (0, 768, 256), (1, 768, 128), (1, 896, 128))


def capacity_rows(tok_rows, top_k, n_exp):
    return max(8, ((5 * top_k * tok_rows) // (4 * n_exp) + 7) // 8 * 8)


def after(value, *earlier):
    return lax.optimization_barrier((value, earlier))[0]


def any_spec():
    return pl.BlockSpec(memory_space=pl.ANY)


def pack_body(n_local, local, n_blk, n_group, first_ref, slot_ref, x_ref, *refs):
    out_refs, acc_ref = refs[:n_group], refs[n_group]
    e, s = pl.program_id(0) * n_local + local, pl.program_id(1)
    count = first_ref[e * (n_blk + 1) + n_blk]
    base = s * TILE

    @pl.when(base < count)
    def _():
        end = jnp.minimum(base + TILE, count)
        lo = jnp.int32(0)
        hi = jnp.int32(0)
        for i in range(n_blk):
            lo += (first_ref[e * (n_blk + 1) + i + 1] <= base).astype(I32)
            hi += (first_ref[e * (n_blk + 1) + i] < end).astype(I32)
        acc_ref[...] = jnp.zeros_like(acc_ref)
        slots = base + lax.broadcasted_iota(I32, (TILE, TOK_BLOCK), 0)

        def visit(i, carry):
            off = pl.multiple_of(i * TOK_BLOCK, TOK_BLOCK)
            pick = (slots == slot_ref[pl.ds(e, 1), pl.ds(off, TOK_BLOCK)]).astype(F32).astype(BF16)
            acc_ref[...] += jnp.dot(pick, x_ref[pl.ds(off, TOK_BLOCK), :], preferred_element_type=F32)
            return carry

        lax.fori_loop(lo, hi, visit, 0)
        for d in range(n_group):

            @pl.when(pl.program_id(0) == d)
            def _():
                out_refs[d][...] = acc_ref[...].astype(BF16)


def pack_rows(first_blk, x_loc, slot_te, n_exp, n_local, local, capacity):
    tok_rows, d_model = x_loc.shape
    n_blk = tok_rows // TOK_BLOCK
    n_group = n_exp // n_local

    def out_spec(d):
        def index(p, s, first):
            used = (first[(d * n_local + local) * (n_blk + 1) + n_blk] + TILE - 1) // TILE
            last = jnp.maximum(used - 1, 0)
            return jnp.where(p < d, 0, jnp.where(p > d, last, jnp.minimum(s, last))), 0

        return pl.BlockSpec((TILE, d_model), index)

    return pl.pallas_call(
        functools.partial(pack_body, n_local, local, n_blk, n_group),
        grid_spec=pltpu.PrefetchScalarGridSpec(
            num_scalar_prefetch=1,
            grid=(n_group, capacity // TILE),
            in_specs=[
                pl.BlockSpec((n_exp, tok_rows), lambda p, s, f: (0, 0)),
                pl.BlockSpec((tok_rows, d_model), lambda p, s, f: (0, 0)),
            ],
            out_specs=[out_spec(d) for d in range(n_group)],
            scratch_shapes=[pltpu.VMEM((TILE, d_model), F32)],
        ),
        out_shape=[jax.ShapeDtypeStruct((capacity, d_model), BF16)] * n_group,
        compiler_params=pltpu.CompilerParams(vmem_limit_bytes=VMEM_LIMIT),
        cost_estimate=pl.CostEstimate(flops=20_000_000_000, bytes_accessed=60_000_000, transcendentals=0),
        name="pack_rows",
    )(first_blk, slot_te, x_loc)


def smem():
    return pl.BlockSpec(memory_space=pltpu.SMEM)


def tile_at(i):
    return pl.ds(pl.multiple_of(i * TILE, TILE), TILE)


def wide_body(n_group, n_far, local, lo_col, cols, meta_ref, *refs):
    x_refs = refs[:n_group]
    wg_ref, wu_ref = refs[n_group : n_group + 2]
    far_refs = refs[n_group + 2 : n_group + 2 + n_far]
    far_g, far_u = far_refs if n_far == 2 else (far_refs[0].at[0], far_refs[0].at[1])
    h_ref, rows_buf, h_buf, gate_w, up_w, row_sems, h_sems, sems = refs[-8:]
    side = meta_ref[0]
    half = wg_ref.shape[1]
    n_live = meta_ref[1 + n_group]

    def fetch(i):
        for d in range(n_group):

            @pl.when((i >= meta_ref[1 + d]) & (i < meta_ref[2 + d]))
            def _():
                pltpu.make_async_copy(x_refs[d].at[tile_at(i - meta_ref[1 + d]), :], rows_buf.at[i % 2], row_sems.at[i % 2]).start()

    def send(i):
        return pltpu.make_async_copy(h_buf.at[i % 2], h_ref.at[tile_at(i), pl.ds(lo_col, cols)], h_sems.at[i % 2])

    fetch(0)
    near = pl.ds(pl.multiple_of(side * half, half), half)
    far = pl.ds(pl.multiple_of((1 - side) * half, half), half)
    copies = [
        pltpu.make_async_copy(wg_ref.at[local, :, pl.ds(lo_col, cols)], gate_w.at[near, :], sems.at[0]),
        pltpu.make_async_copy(wu_ref.at[local, :, pl.ds(lo_col, cols)], up_w.at[near, :], sems.at[1]),
        pltpu.make_async_copy(far_g, gate_w.at[far, :], sems.at[2]),
        pltpu.make_async_copy(far_u, up_w.at[far, :], sems.at[3]),
    ]
    for copy in copies:
        copy.start()
    for copy in copies:
        copy.wait()

    def step(i, carry):
        fetch(i + 1)
        pltpu.make_async_copy(x_refs[0].at[tile_at(0), :], rows_buf.at[i % 2], row_sems.at[i % 2]).wait()

        @pl.when(i >= 2)
        def _():
            send(i - 2).wait()

        def part(j, carry):
            span = pl.ds(pl.multiple_of(j * SUB, SUB), SUB)
            rows = rows_buf[i % 2]
            g = jnp.dot(rows, gate_w[:, span], preferred_element_type=F32)
            u = jnp.dot(rows, up_w[:, span], preferred_element_type=F32)
            h_buf[i % 2, :, span] = (jax.nn.silu(g) * u).astype(BF16)
            return carry

        lax.fori_loop(0, cols // SUB, part, 0)
        send(i).start()
        return carry

    lax.fori_loop(0, n_live, step, 0)
    for back in (2, 1):

        @pl.when(n_live >= back)
        def _():
            send(n_live - back).wait()


def wide_part(meta, hidden, rows, w_gate, w_up, far, local, lo_col, cols):
    n_group = len(rows)
    capacity, d_model = rows[0].shape
    n_rows = n_group * capacity
    ffn = w_gate.shape[2]
    far = far if isinstance(far, list) else [far]
    args = [meta, *rows, w_gate, w_up, *far]
    alias = {}
    if hidden is not None:
        alias = {len(args): 0}
        args.append(hidden)
    return pl.pallas_call(
        functools.partial(wide_body, n_group, len(far), local, lo_col, cols),
        in_specs=[smem()] + [any_spec()] * (len(args) - 1),
        out_specs=any_spec(),
        scratch_shapes=[
            pltpu.VMEM((2, TILE, d_model), BF16),
            pltpu.VMEM((2, TILE, cols), BF16),
            pltpu.VMEM((d_model, cols), BF16),
            pltpu.VMEM((d_model, cols), BF16),
            pltpu.SemaphoreType.DMA((2,)),
            pltpu.SemaphoreType.DMA((2,)),
            pltpu.SemaphoreType.DMA((4,)),
        ],
        out_shape=jax.ShapeDtypeStruct((n_rows, ffn), BF16),
        input_output_aliases=alias,
        compiler_params=pltpu.CompilerParams(vmem_limit_bytes=VMEM_LIMIT),
        cost_estimate=pl.CostEstimate(flops=4 * n_rows * d_model * cols, bytes_accessed=n_rows * d_model * 2, transcendentals=0),
        name="wide_part",
    )(*args)


def down_body(segs, local, deep, pair_size, n_hidden, meta_ref, *refs):
    h_refs, w_ref, refs = refs[:n_hidden], refs[n_hidden], refs[n_hidden + 1 :]
    out_refs = refs[: len(segs)]
    h_buf, out_buf, w_buf, h_sems, out_sems, sem = refs[len(segs) :]
    begin = meta_ref[1 + segs[0]]
    n_live = meta_ref[2 + segs[-1]] - begin
    block = min(w_buf.shape[1], DOWN_BLOCK)

    def fetch(i):
        for l, h_ref in enumerate(h_refs):
            copy = pltpu.make_async_copy(h_ref.at[tile_at(begin + i), :], h_buf.at[i % deep], h_sems.at[i % deep])
            if n_hidden == 1:
                copy.start()
            else:
                pl.when(meta_ref[0] == l)(copy.start)

    def fetched(i):
        pltpu.make_async_copy(h_refs[0].at[tile_at(0), :], h_buf.at[i % deep], h_sems.at[i % deep]).wait()

    def sent(i):
        pltpu.make_async_copy(out_buf.at[i % deep], out_refs[0].at[tile_at(0), :], out_sems.at[i % deep]).wait()

    def send(i, there, tile):
        pltpu.make_async_copy(out_buf.at[i % deep], there.at[tile_at(tile), :], out_sems.at[i % deep]).start()

    copy = pltpu.make_async_copy(w_ref if local is None else w_ref.at[local], w_buf, sem)
    copy.start()
    for i in range(deep - pair_size):

        @pl.when(i < n_live)
        def _():
            fetch(i)

    copy.wait()

    def step(pair, carry):
        for k in range(pair_size):
            i = pair * pair_size + k

            @pl.when(i + deep - pair_size < n_live)
            def _():
                fetch(i + deep - pair_size)

        for k in range(pair_size):
            i = pair * pair_size + k

            @pl.when(i < n_live)
            def _():
                fetched(i)

            @pl.when((i >= deep) & (i - deep < n_live))
            def _():
                sent(i)

        slots = pl.ds(pair % (deep // pair_size) * pair_size, pair_size)

        def part(j, carry):
            span = pl.ds(pl.multiple_of(j * block, block), block)
            total = jnp.dot(h_buf[slots].reshape(pair_size * TILE, -1), w_buf[:, span], preferred_element_type=F32)
            out_buf[slots, :, span] = total.astype(BF16).reshape(pair_size, TILE, -1)
            return carry

        lax.fori_loop(0, w_buf.shape[1] // block, part, 0)
        for k in range(pair_size):
            i = pair * pair_size + k
            for d, out_ref in zip(segs, out_refs):

                @pl.when((begin + i >= meta_ref[1 + d]) & (begin + i < meta_ref[2 + d]))
                def _():
                    send(i, out_ref, begin + i - meta_ref[1 + d])

        return carry

    n_pair = (n_live + pair_size - 1) // pair_size
    lax.fori_loop(0, n_pair, step, 0)
    for back in range(deep, 0, -1):
        i = n_pair * pair_size - back

        @pl.when((i >= 0) & (i < n_live))
        def _():
            sent(i)

    for d, out_ref in zip(segs, out_refs):
        @pl.when(meta_ref[1 + d] == meta_ref[2 + d])
        def _():
            out_buf[0] = jnp.zeros_like(out_buf[0])
            send(0, out_ref, 0)
            sent(0)


def down_part(meta, hidden, weight, n_group, local=None, segs=None):
    segs = tuple(range(n_group)) if segs is None else segs
    n_rows = hidden[0].shape[0]
    n_hid, width = weight.shape[-2:]
    deep, pair_size = 4, 1
    return pl.pallas_call(
        functools.partial(down_body, segs, local, deep, pair_size, len(hidden)),
        in_specs=[smem()] + [any_spec()] * (len(hidden) + 1),
        out_specs=[any_spec()] * len(segs),
        scratch_shapes=[
            pltpu.VMEM((deep, TILE, n_hid), BF16),
            pltpu.VMEM((deep, TILE, width), BF16),
            pltpu.VMEM((n_hid, width), BF16),
            pltpu.SemaphoreType.DMA((deep,)),
            pltpu.SemaphoreType.DMA((deep,)),
            pltpu.SemaphoreType.DMA,
        ],
        out_shape=[jax.ShapeDtypeStruct((n_rows // n_group, width), BF16)] * len(segs),
        compiler_params=pltpu.CompilerParams(vmem_limit_bytes=VMEM_LIMIT),
        cost_estimate=pl.CostEstimate(flops=2 * n_rows * n_hid * width, bytes_accessed=n_rows * n_hid * 2, transcendentals=0),
        name="down_part",
    )(meta, *hidden, weight)


def mix_body(n_exp, n_tile, subs, widths, unroll, col_ref, chunk_ref, pos_ref, gate_ref, x_ref, *refs):
    n_set = len(widths)
    back_refs = refs[: n_set * n_exp]
    y_ref, mark_ref, pos_buf, gate_buf = refs[-6 - 4 * n_set : -2 - 4 * n_set]
    bufs, sems, y_sems = refs[-2 - 4 * n_set : -2], refs[-2], refs[-1]
    sets = []
    copies = [pltpu.make_async_copy(pos_ref, pos_buf, sems.at[0]), pltpu.make_async_copy(gate_ref, gate_buf, sems.at[1])]
    for g, width in enumerate(widths):
        back_buf, near_buf, x_buf, y_buf = bufs[4 * g : 4 * g + 4]
        cols = pl.ds(pl.multiple_of(col_ref[g], 128), width)
        sets.append((back_buf, near_buf, x_buf, y_buf, cols))
        for e in range(n_exp):
            ref, sub = back_refs[g * n_exp + e], subs[g * n_exp + e]
            capacity = ref.shape[0]
            here = back_buf.at[pl.ds(e * capacity, capacity), :]
            copies.append(pltpu.make_async_copy(ref.at[:, pl.ds(sub * width, width)], here, sems.at[len(copies)]))
        copies.append(pltpu.make_async_copy(x_ref.at[:, cols], x_buf, sems.at[len(copies)]))
    for copy in copies:
        copy.start()
    for copy in copies:
        copy.wait()

    def out(g, block):
        _, _, _, y_buf, cols = sets[g]
        rows = pl.ds(pl.multiple_of(block * (unroll * MIX_TILE), unroll * MIX_TILE), unroll * MIX_TILE)
        return pltpu.make_async_copy(y_buf.at[rows, :], y_ref.at[rows, cols], y_sems.at[g, block])

    def step(block, carry):
        for k in range(unroll):
            i = block * unroll + k
            tokens = pl.ds(pl.multiple_of(i * MIX_TILE, MIX_TILE), MIX_TILE)
            seat = lax.broadcasted_iota(I32, (MIX_TILE, REACH), 1)
            pick = jnp.concatenate([(seat == pos_buf[tokens, j : j + 1]).astype(F32).astype(BF16) for j in range(2)], axis=0)
            for back_buf, near_buf, x_buf, y_buf, _ in sets:
                for c in range(REACH // ALIGN):
                    chunk = pl.multiple_of(chunk_ref[i * (REACH // ALIGN) + c], ALIGN)
                    near_buf[k, c * ALIGN : (c + 1) * ALIGN, :] = back_buf[pl.ds(chunk, ALIGN), :]
                found = jnp.dot(pick, near_buf[k], preferred_element_type=F32)
                mixed = gate_buf[tokens, 0:1] * found[:MIX_TILE] + gate_buf[tokens, 1:2] * found[MIX_TILE:]
                y_buf[tokens, :] = (x_buf[tokens, :].astype(F32) + mixed).astype(BF16)
        for g in range(n_set):
            out(g, block).start()
        return carry

    lax.fori_loop(0, n_tile // unroll, step, 0)
    for block in range(n_tile // unroll):
        for g in range(n_set):
            out(g, block).wait()
    mark_ref[0] = 0


def mix_cols(col, y_loc, x_loc, pos, gate_loc, chunks, widths, back):
    tok_rows, d_model = x_loc.shape
    n_exp = len(back) // len(widths)
    capacity = back[0][0].shape[0]
    unroll = 4 if sum(widths) < 256 else 2
    args = [col, chunks, pos, gate_loc, x_loc, *[array for array, _ in back]]
    specs = [smem(), smem()] + [any_spec()] * (3 + len(back))
    alias = {}
    if y_loc is not None:
        alias = {len(args): 0}
        args.append(y_loc)
        specs.append(any_spec())
    bufs = [pltpu.VMEM(pos.shape, I32), pltpu.VMEM(gate_loc.shape, F32)]
    for width in widths:
        bufs += [
            pltpu.VMEM((n_exp * capacity, width), BF16),
            pltpu.VMEM((unroll, REACH, width), BF16),
            pltpu.VMEM((tok_rows, width), BF16),
            pltpu.VMEM((tok_rows, width), BF16),
        ]
    return pl.pallas_call(
        functools.partial(mix_body, n_exp, tok_rows // MIX_TILE, tuple(sub for _, sub in back), widths, unroll),
        in_specs=specs,
        out_specs=[any_spec(), smem()],
        scratch_shapes=bufs
        + [
            pltpu.SemaphoreType.DMA((2 + (n_exp + 1) * len(widths),)),
            pltpu.SemaphoreType.DMA((len(widths), tok_rows // MIX_TILE // unroll)),
        ],
        out_shape=[jax.ShapeDtypeStruct((tok_rows, d_model), BF16), jax.ShapeDtypeStruct((1,), I32)],
        input_output_aliases=alias,
        compiler_params=pltpu.CompilerParams(vmem_limit_bytes=VMEM_LIMIT),
        cost_estimate=pl.CostEstimate(flops=20_000_000 * sum(widths), bytes_accessed=20_000 * sum(widths), transcendentals=0),
        name="mix_cols",
    )(*args)


def spans(sizes):
    lo = 0
    for size in sizes:
        yield lo, size
        lo += size


def solution(mesh):
    n_group, n_side = mesh.shape["expert"], mesh.shape["data"]
    tok_spec = P(("rep", "expert", "data"), None)
    wide_spec = P("expert", "data", None)
    down_spec = P("expert", None, "data")
    swap = [(s, 1 - s) for s in range(n_side)]

    def whole_step(x_loc, idx_loc, gate_loc, wg_loc, wu_loc, wd_loc):
        tok_rows, _ = x_loc.shape
        top_k = idx_loc.shape[1]
        n_local, half, ffn = wg_loc.shape
        n_exp = n_local * n_group
        capacity = capacity_rows(tok_rows, top_k, n_exp)
        side = lax.axis_index("data")
        place = lax.axis_index("expert")
        locals_ = range(n_local)
        groups = jnp.arange(n_group, dtype=I32)

        ids = ((idx_loc // n_local + n_group - place) % n_group * n_local + idx_loc % n_local).T
        experts = jnp.arange(n_exp, dtype=I32)[:, None]
        chosen = functools.reduce(jnp.logical_or, [ids[j][None, :] == experts for j in range(top_k)])
        chosen_i = chosen.astype(I32)
        running = jnp.cumsum(chosen_i, axis=1)
        before = running - chosen_i
        slot_te = jnp.where(chosen & (before < capacity), before, -1)
        counts = jnp.minimum(running[:, -1], capacity)
        first = jnp.minimum(before, capacity)
        first_blk = jnp.concatenate([first[:, ::TOK_BLOCK], counts[:, None]], axis=1).reshape(-1)
        first_mix = first[:, ::MIX_TILE]

        table = lax.all_gather(counts, "expert")
        meta = []
        for l in locals_:
            mine = jnp.sum(jnp.where(((place - groups) % n_group)[:, None, None] == groups[None, :, None], table.reshape(n_group, n_group, n_local)[None, :, :, l] * (groups[:, None, None] == groups[None, None, :]), 0), axis=(1, 2))
            ends = jnp.cumsum((mine + TILE - 1) // TILE)
            meta.append(jnp.concatenate([side[None], jnp.zeros((1,), I32), ends]).astype(I32))

        reach = REACH // ALIGN
        start = first_mix // ALIGN
        stop = jnp.concatenate([first_mix[:, 1:], counts[:, None]], axis=1)
        size = jnp.where(stop > first_mix, (stop + ALIGN - 1) // ALIGN - start, 0)
        lead = jnp.cumsum(size, axis=0) - size
        at = slot_te + jnp.repeat((lead - start) * ALIGN, MIX_TILE, axis=1)
        at = jnp.where(slot_te < 0, -1, at)
        pos = jnp.stack([jnp.sum(jnp.where(ids[j][None, :] == experts, at, 0), axis=0) for j in range(top_k)], axis=1)
        seat = jnp.arange(reach, dtype=I32)[None, None, :]
        taken = (seat >= lead[:, :, None]) & (seat < (lead + size)[:, :, None])

        def chunk_table(array):
            source = array[:, :, None] * (capacity // ALIGN) + (start - lead)[:, :, None] + seat
            return (jnp.sum(jnp.where(taken, source, 0), axis=0) * ALIGN).reshape(-1)

        chunks = chunk_table(experts)

        done = []

        def in_turn(kernel, small, *args, follows=True):
            if done and follows:
                small = after(small, done[-1]) if done[-1].ndim else small + done[-1]
            out = kernel(small, *args)
            done.append(out[0] if isinstance(out, (list, tuple)) else out)
            return out

        wide_spans = list(spans(WIDE_CHUNKS))
        parts = [[w[0, :, : wide_spans[0][1]] for w in (wg_loc, wu_loc)]]
        later = after((wg_loc, wu_loc), parts[0])
        parts += [jnp.stack([w[l, :, lo : lo + n] for w in later]) for l in locals_ for lo, n in wide_spans if l or lo]
        far = []

        def cross():
            if len(far) == len(parts):
                return
            piece = parts[len(far)]
            if len(far) >= 2:
                piece = after(piece, far[-2])
            far.append(lax.ppermute(piece, "data", swap))

        def exchange(blocks, step):
            out = [blocks[0]]
            for d in range(1, n_group):
                out.append(lax.ppermute(blocks[d], "expert", [(s, (s + step * d) % n_group) for s in range(n_group)]))
            return out

        def mix(y_loc, chunks, *sets):
            col = jnp.stack([col for col, _, _ in sets]).astype(I32)
            back = [(pair[l][0][d], pair[l][1]) for _, _, pair in sets for d in range(n_group) for l in locals_]
            out = in_turn(mix_cols, col, y_loc, x_loc, pos, gate_loc, chunks, tuple(width for _, width, _ in sets), back)
            done[-1] = out[1][0]
            return out[0]

        cross()
        cross()
        first_blk = after(first_blk, meta)
        rows = [exchange(in_turn(pack_rows, first_blk, x_loc, slot_te, n_exp, n_local, 0, capacity), 1)]
        cross()
        packed = in_turn(pack_rows, first_blk, x_loc, slot_te, n_exp, n_local, 1, capacity)
        cross()
        rows.append(exchange([after(block, rows[0]) for block in packed], 1))

        n_wide = len(wide_spans)
        hidden, own = [], []
        for l in locals_:
            hidden.append(None)
            for k, (lo, n) in enumerate(wide_spans):
                if k >= 2 or (l and k):
                    cross()
                hidden[l] = in_turn(wide_part, meta[l], hidden[l], rows[l], wg_loc, wu_loc, far[l * n_wide + k], l, lo, n, follows=k == 0)
                if not (l or k):
                    at_group = (groups[:, None, None] + groups[None, :, None]) % n_group == groups[None, None, :]
                    held = table.reshape(n_group, n_group, 1, n_local)
                    totals = after(jnp.sum(jnp.where(at_group[..., None], held, 0), axis=(0, 1)), done[-1])
                    totals += lax.ppermute(totals, "data", swap)
            if l == 0:
                cross()
                flips = (totals[:, 1] > totals[:, 0]).astype(I32)
                flip = jnp.sum(jnp.where(groups == place, flips, 0))
                parts += [lax.dynamic_slice(wd_loc, ((r + flip) % n_local, 0, lo), (1, ffn, n))[0] for r, lo, n in DOWN_PIECES]
            own.append(exchange(in_turn(down_part, meta[l], [hidden[l]], wd_loc, n_group, l, follows=False), -1))

        role_meta = []
        for r in locals_:
            picked = jnp.where(flip == 1, meta[(r + 1) % n_local], meta[r])
            role_meta.append(jnp.concatenate([((r + flip) % n_local)[None], picked[1:]]))
        d_flips = jnp.sum(jnp.where(((place + groups) % n_group)[:, None] == groups[None, :], flips[None, :], 0), axis=1)
        roles = (jnp.arange(n_local, dtype=I32)[None, :] + d_flips[:, None]) % n_local
        far_chunks = chunk_table((groups[:, None] * n_local + roles).reshape(n_exp, 1))

        def far_piece(i):
            cross()
            r = DOWN_PIECES[i][0]
            return exchange(in_turn(down_part, role_meta[r], hidden, far[n_local * n_wide + i], n_group), -1)

        far_col = (1 - side) * half
        ret = [far_piece(0), far_piece(1)]
        y_loc = mix(None, chunks, (side * half, half, [(own[l], 0) for l in locals_]))
        ret += [far_piece(2), far_piece(3)]
        y_loc = mix(y_loc, far_chunks, (far_col, 512, [(ret[0], 0), (ret[1], 0)]))
        ret.append(far_piece(4))
        y_loc = mix(y_loc, far_chunks, (far_col + 512, 256, [(ret[2], 0), (ret[3], 0)]))
        ret += [far_piece(5), far_piece(6)]
        y_loc = mix(y_loc, far_chunks, (far_col + 768, 128, [(ret[4], 0), (ret[5], 0)]))
        return mix(y_loc, far_chunks, (far_col + 896, 128, [(ret[4], 1), (ret[6], 0)]))

    in_specs = (tok_spec, tok_spec, tok_spec, wide_spec, wide_spec, down_spec)
    return jax.shard_map(whole_step, mesh=mesh, in_specs=in_specs, out_specs=tok_spec, check_vma=False)
```

```python
import functools

import jax
import jax.numpy as jnp
from jax import lax
from jax.experimental import pallas as pl
from jax.experimental.pallas import tpu as pltpu
from jax.sharding import PartitionSpec as P


BF16 = jnp.bfloat16
F32 = jnp.float32
I32 = jnp.int32
VMEM_LIMIT = 66_000_000

TILE = 256
TOK_BLOCK = 256
MIX_TILE = 128
ALIGN = 16
REACH = 512
DOWN_BLOCK = 512
SUB = 512
WIDE_CHUNKS = (512, 2048, 1536, 1536)
DOWN_PIECES = ((0, 0, 512), (1, 0, 512), (0, 512, 256), (1, 512, 256), (0, 768, 256), (1, 768, 128), (1, 896, 128))


def capacity_rows(tok_rows, top_k, n_exp):
    return max(8, ((5 * top_k * tok_rows) // (4 * n_exp) + 7) // 8 * 8)


def after(value, *earlier):
    return lax.optimization_barrier((value, earlier))[0]


def any_spec():
    return pl.BlockSpec(memory_space=pl.ANY)


def pack_body(n_local, local, n_blk, n_group, first_ref, slot_ref, x_ref, *refs):
    out_refs, acc_ref = refs[:n_group], refs[n_group]
    e, s = pl.program_id(0) * n_local + local, pl.program_id(1)
    count = first_ref[e * (n_blk + 1) + n_blk]
    base = s * TILE

    @pl.when(base < count)
    def _():
        end = jnp.minimum(base + TILE, count)
        lo = jnp.int32(0)
        hi = jnp.int32(0)
        for i in range(n_blk):
            lo += (first_ref[e * (n_blk + 1) + i + 1] <= base).astype(I32)
            hi += (first_ref[e * (n_blk + 1) + i] < end).astype(I32)
        acc_ref[...] = jnp.zeros_like(acc_ref)
        slots = base + lax.broadcasted_iota(I32, (TILE, TOK_BLOCK), 0)

        def visit(i, carry):
            off = pl.multiple_of(i * TOK_BLOCK, TOK_BLOCK)
            pick = (slots == slot_ref[pl.ds(e, 1), pl.ds(off, TOK_BLOCK)]).astype(F32).astype(BF16)
            acc_ref[...] += jnp.dot(pick, x_ref[pl.ds(off, TOK_BLOCK), :], preferred_element_type=F32)
            return carry

        lax.fori_loop(lo, hi, visit, 0)
        for d in range(n_group):

            @pl.when(pl.program_id(0) == d)
            def _():
                out_refs[d][...] = acc_ref[...].astype(BF16)


def pack_rows(first_blk, x_loc, slot_te, n_exp, n_local, local, capacity):
    tok_rows, d_model = x_loc.shape
    n_blk = tok_rows // TOK_BLOCK
    n_group = n_exp // n_local

    def out_spec(d):
        def index(p, s, first):
            used = (first[(d * n_local + local) * (n_blk + 1) + n_blk] + TILE - 1) // TILE
            last = jnp.maximum(used - 1, 0)
            return jnp.where(p < d, 0, jnp.where(p > d, last, jnp.minimum(s, last))), 0

        return pl.BlockSpec((TILE, d_model), index)

    return pl.pallas_call(
        functools.partial(pack_body, n_local, local, n_blk, n_group),
        grid_spec=pltpu.PrefetchScalarGridSpec(
            num_scalar_prefetch=1,
            grid=(n_group, capacity // TILE),
            in_specs=[
                pl.BlockSpec((n_exp, tok_rows), lambda p, s, f: (0, 0)),
                pl.BlockSpec((tok_rows, d_model), lambda p, s, f: (0, 0)),
            ],
            out_specs=[out_spec(d) for d in range(n_group)],
            scratch_shapes=[pltpu.VMEM((TILE, d_model), F32)],
        ),
        out_shape=[jax.ShapeDtypeStruct((capacity, d_model), BF16)] * n_group,
        compiler_params=pltpu.CompilerParams(vmem_limit_bytes=VMEM_LIMIT),
        cost_estimate=pl.CostEstimate(flops=20_000_000_000, bytes_accessed=60_000_000, transcendentals=0),
        name="pack_rows",
    )(first_blk, slot_te, x_loc)


def smem():
    return pl.BlockSpec(memory_space=pltpu.SMEM)


def tile_at(i):
    return pl.ds(pl.multiple_of(i * TILE, TILE), TILE)


def wide_body(n_group, n_far, local, lo_col, cols, meta_ref, *refs):
    x_refs = refs[:n_group]
    wg_ref, wu_ref = refs[n_group : n_group + 2]
    far_refs = refs[n_group + 2 : n_group + 2 + n_far]
    far_g, far_u = far_refs if n_far == 2 else (far_refs[0].at[0], far_refs[0].at[1])
    h_ref, rows_buf, h_buf, gate_w, up_w, row_sems, h_sems, sems = refs[-8:]
    side = meta_ref[0]
    half = wg_ref.shape[1]
    n_live = meta_ref[1 + n_group]

    def fetch(i):
        for d in range(n_group):

            @pl.when((i >= meta_ref[1 + d]) & (i < meta_ref[2 + d]))
            def _():
                pltpu.make_async_copy(x_refs[d].at[tile_at(i - meta_ref[1 + d]), :], rows_buf.at[i % 2], row_sems.at[i % 2]).start()

    def send(i):
        return pltpu.make_async_copy(h_buf.at[i % 2], h_ref.at[tile_at(i), pl.ds(lo_col, cols)], h_sems.at[i % 2])

    fetch(0)
    near = pl.ds(pl.multiple_of(side * half, half), half)
    far = pl.ds(pl.multiple_of((1 - side) * half, half), half)
    copies = [
        pltpu.make_async_copy(wg_ref.at[local, :, pl.ds(lo_col, cols)], gate_w.at[near, :], sems.at[0]),
        pltpu.make_async_copy(wu_ref.at[local, :, pl.ds(lo_col, cols)], up_w.at[near, :], sems.at[1]),
        pltpu.make_async_copy(far_g, gate_w.at[far, :], sems.at[2]),
        pltpu.make_async_copy(far_u, up_w.at[far, :], sems.at[3]),
    ]
    for copy in copies:
        copy.start()
    for copy in copies:
        copy.wait()

    def step(i, carry):
        fetch(i + 1)
        pltpu.make_async_copy(x_refs[0].at[tile_at(0), :], rows_buf.at[i % 2], row_sems.at[i % 2]).wait()

        @pl.when(i >= 2)
        def _():
            send(i - 2).wait()

        def part(j, carry):
            span = pl.ds(pl.multiple_of(j * SUB, SUB), SUB)
            rows = rows_buf[i % 2]
            g = jnp.dot(rows, gate_w[:, span], preferred_element_type=F32)
            u = jnp.dot(rows, up_w[:, span], preferred_element_type=F32)
            h_buf[i % 2, :, span] = (jax.nn.silu(g) * u).astype(BF16)
            return carry

        lax.fori_loop(0, cols // SUB, part, 0)
        send(i).start()
        return carry

    lax.fori_loop(0, n_live, step, 0)
    for back in (2, 1):

        @pl.when(n_live >= back)
        def _():
            send(n_live - back).wait()


def wide_part(meta, hidden, rows, w_gate, w_up, far, local, lo_col, cols):
    n_group = len(rows)
    capacity, d_model = rows[0].shape
    n_rows = n_group * capacity
    ffn = w_gate.shape[2]
    far = far if isinstance(far, list) else [far]
    args = [meta, *rows, w_gate, w_up, *far]
    alias = {}
    if hidden is not None:
        alias = {len(args): 0}
        args.append(hidden)
    return pl.pallas_call(
        functools.partial(wide_body, n_group, len(far), local, lo_col, cols),
        in_specs=[smem()] + [any_spec()] * (len(args) - 1),
        out_specs=any_spec(),
        scratch_shapes=[
            pltpu.VMEM((2, TILE, d_model), BF16),
            pltpu.VMEM((2, TILE, cols), BF16),
            pltpu.VMEM((d_model, cols), BF16),
            pltpu.VMEM((d_model, cols), BF16),
            pltpu.SemaphoreType.DMA((2,)),
            pltpu.SemaphoreType.DMA((2,)),
            pltpu.SemaphoreType.DMA((4,)),
        ],
        out_shape=jax.ShapeDtypeStruct((n_rows, ffn), BF16),
        input_output_aliases=alias,
        compiler_params=pltpu.CompilerParams(vmem_limit_bytes=VMEM_LIMIT),
        cost_estimate=pl.CostEstimate(flops=4 * n_rows * d_model * cols, bytes_accessed=n_rows * d_model * 2, transcendentals=0),
        name="wide_part",
    )(*args)


def down_body(segs, local, deep, pair_size, n_hidden, meta_ref, *refs):
    h_refs, w_ref, refs = refs[:n_hidden], refs[n_hidden], refs[n_hidden + 1 :]
    out_refs = refs[: len(segs)]
    h_buf, out_buf, w_buf, h_sems, out_sems, sem = refs[len(segs) :]
    begin = meta_ref[1 + segs[0]]
    n_live = meta_ref[2 + segs[-1]] - begin
    block = min(w_buf.shape[1], DOWN_BLOCK)

    def fetch(i):
        for l, h_ref in enumerate(h_refs):
            copy = pltpu.make_async_copy(h_ref.at[tile_at(begin + i), :], h_buf.at[i % deep], h_sems.at[i % deep])
            if n_hidden == 1:
                copy.start()
            else:
                pl.when(meta_ref[0] == l)(copy.start)

    def fetched(i):
        pltpu.make_async_copy(h_refs[0].at[tile_at(0), :], h_buf.at[i % deep], h_sems.at[i % deep]).wait()

    def sent(i):
        pltpu.make_async_copy(out_buf.at[i % deep], out_refs[0].at[tile_at(0), :], out_sems.at[i % deep]).wait()

    def send(i, there, tile):
        pltpu.make_async_copy(out_buf.at[i % deep], there.at[tile_at(tile), :], out_sems.at[i % deep]).start()

    copy = pltpu.make_async_copy(w_ref if local is None else w_ref.at[local], w_buf, sem)
    copy.start()
    for i in range(deep - pair_size):

        @pl.when(i < n_live)
        def _():
            fetch(i)

    copy.wait()

    def step(pair, carry):
        for k in range(pair_size):
            i = pair * pair_size + k

            @pl.when(i + deep - pair_size < n_live)
            def _():
                fetch(i + deep - pair_size)

        for k in range(pair_size):
            i = pair * pair_size + k

            @pl.when(i < n_live)
            def _():
                fetched(i)

            @pl.when((i >= deep) & (i - deep < n_live))
            def _():
                sent(i)

        slots = pl.ds(pair % (deep // pair_size) * pair_size, pair_size)

        def part(j, carry):
            span = pl.ds(pl.multiple_of(j * block, block), block)
            total = jnp.dot(h_buf[slots].reshape(pair_size * TILE, -1), w_buf[:, span], preferred_element_type=F32)
            out_buf[slots, :, span] = total.astype(BF16).reshape(pair_size, TILE, -1)
            return carry

        lax.fori_loop(0, w_buf.shape[1] // block, part, 0)
        for k in range(pair_size):
            i = pair * pair_size + k
            for d, out_ref in zip(segs, out_refs):

                @pl.when((begin + i >= meta_ref[1 + d]) & (begin + i < meta_ref[2 + d]))
                def _():
                    send(i, out_ref, begin + i - meta_ref[1 + d])

        return carry

    n_pair = (n_live + pair_size - 1) // pair_size
    lax.fori_loop(0, n_pair, step, 0)
    for back in range(deep, 0, -1):
        i = n_pair * pair_size - back

        @pl.when((i >= 0) & (i < n_live))
        def _():
            sent(i)

    for d, out_ref in zip(segs, out_refs):
        @pl.when(meta_ref[1 + d] == meta_ref[2 + d])
        def _():
            out_buf[0] = jnp.zeros_like(out_buf[0])
            send(0, out_ref, 0)
            sent(0)


def down_part(meta, hidden, weight, n_group, local=None, segs=None):
    segs = tuple(range(n_group)) if segs is None else segs
    n_rows = hidden[0].shape[0]
    n_hid, width = weight.shape[-2:]
    deep, pair_size = 4, 1
    return pl.pallas_call(
        functools.partial(down_body, segs, local, deep, pair_size, len(hidden)),
        in_specs=[smem()] + [any_spec()] * (len(hidden) + 1),
        out_specs=[any_spec()] * len(segs),
        scratch_shapes=[
            pltpu.VMEM((deep, TILE, n_hid), BF16),
            pltpu.VMEM((deep, TILE, width), BF16),
            pltpu.VMEM((n_hid, width), BF16),
            pltpu.SemaphoreType.DMA((deep,)),
            pltpu.SemaphoreType.DMA((deep,)),
            pltpu.SemaphoreType.DMA,
        ],
        out_shape=[jax.ShapeDtypeStruct((n_rows // n_group, width), BF16)] * len(segs),
        compiler_params=pltpu.CompilerParams(vmem_limit_bytes=VMEM_LIMIT),
        cost_estimate=pl.CostEstimate(flops=2 * n_rows * n_hid * width, bytes_accessed=n_rows * n_hid * 2, transcendentals=0),
        name="down_part",
    )(meta, *hidden, weight)


def mix_body(n_exp, n_tile, subs, widths, unroll, col_ref, chunk_ref, pair_ref, x_ref, *refs):
    n_set = len(widths)
    back_refs = refs[: n_set * n_exp]
    y_ref, mark_ref, pair_buf = refs[-5 - 4 * n_set : -2 - 4 * n_set]
    bufs, sems, y_sems = refs[-2 - 4 * n_set : -2], refs[-2], refs[-1]
    sets = []
    copies = [pltpu.make_async_copy(pair_ref, pair_buf, sems.at[0])]
    for g, width in enumerate(widths):
        back_buf, near_buf, x_buf, y_buf = bufs[4 * g : 4 * g + 4]
        cols = pl.ds(pl.multiple_of(col_ref[g], 128), width)
        sets.append((back_buf, near_buf, x_buf, y_buf, cols))
        for e in range(n_exp):
            ref, sub = back_refs[g * n_exp + e], subs[g * n_exp + e]
            capacity = ref.shape[0]
            here = back_buf.at[pl.ds(e * capacity, capacity), :]
            copies.append(pltpu.make_async_copy(ref.at[:, pl.ds(sub * width, width)], here, sems.at[len(copies)]))
        copies.append(pltpu.make_async_copy(x_ref.at[:, cols], x_buf, sems.at[len(copies)]))
    for copy in copies:
        copy.start()
    for copy in copies:
        copy.wait()

    def out(g, block):
        _, _, _, y_buf, cols = sets[g]
        rows = pl.ds(pl.multiple_of(block * (unroll * MIX_TILE), unroll * MIX_TILE), unroll * MIX_TILE)
        return pltpu.make_async_copy(y_buf.at[rows, :], y_ref.at[rows, cols], y_sems.at[g, block])

    def step(block, carry):
        for k in range(unroll):
            i = block * unroll + k
            tokens = pl.ds(pl.multiple_of(i * MIX_TILE, MIX_TILE), MIX_TILE)
            seat = lax.broadcasted_iota(I32, (MIX_TILE, REACH), 1)
            pick = jnp.concatenate([(seat == pair_buf[tokens, j : j + 1].astype(I32)).astype(F32).astype(BF16) for j in range(2)], axis=0)
            for back_buf, near_buf, x_buf, y_buf, _ in sets:
                for c in range(REACH // ALIGN):
                    chunk = pl.multiple_of(chunk_ref[i * (REACH // ALIGN) + c], ALIGN)
                    near_buf[k, c * ALIGN : (c + 1) * ALIGN, :] = back_buf[pl.ds(chunk, ALIGN), :]
                found = jnp.dot(pick, near_buf[k], preferred_element_type=F32)
                mixed = pair_buf[tokens, 2:3] * found[:MIX_TILE] + pair_buf[tokens, 3:4] * found[MIX_TILE:]
                y_buf[tokens, :] = (x_buf[tokens, :].astype(F32) + mixed).astype(BF16)
        for g in range(n_set):
            out(g, block).start()
        return carry

    lax.fori_loop(0, n_tile // unroll, step, 0)
    for block in range(n_tile // unroll):
        for g in range(n_set):
            out(g, block).wait()
    mark_ref[0] = 0


def mix_cols(col, y_loc, x_loc, pairs, chunks, widths, back):
    tok_rows, d_model = x_loc.shape
    n_exp = len(back) // len(widths)
    capacity = back[0][0].shape[0]
    unroll = 8 if sum(widths) < 256 else 4 if sum(widths) < 512 else 2
    args = [col, chunks, pairs, x_loc, *[array for array, _ in back]]
    specs = [smem(), smem()] + [any_spec()] * (2 + len(back))
    alias = {}
    if y_loc is not None:
        alias = {len(args): 0}
        args.append(y_loc)
        specs.append(any_spec())
    bufs = [pltpu.VMEM(pairs.shape, F32)]
    for width in widths:
        bufs += [
            pltpu.VMEM((n_exp * capacity, width), BF16),
            pltpu.VMEM((unroll, REACH, width), BF16),
            pltpu.VMEM((tok_rows, width), BF16),
            pltpu.VMEM((tok_rows, width), BF16),
        ]
    return pl.pallas_call(
        functools.partial(mix_body, n_exp, tok_rows // MIX_TILE, tuple(sub for _, sub in back), widths, unroll),
        in_specs=specs,
        out_specs=[any_spec(), smem()],
        scratch_shapes=bufs
        + [
            pltpu.SemaphoreType.DMA((1 + (n_exp + 1) * len(widths),)),
            pltpu.SemaphoreType.DMA((len(widths), tok_rows // MIX_TILE // unroll)),
        ],
        out_shape=[jax.ShapeDtypeStruct((tok_rows, d_model), BF16), jax.ShapeDtypeStruct((1,), I32)],
        input_output_aliases=alias,
        compiler_params=pltpu.CompilerParams(vmem_limit_bytes=VMEM_LIMIT),
        cost_estimate=pl.CostEstimate(flops=20_000_000 * sum(widths), bytes_accessed=20_000 * sum(widths), transcendentals=0),
        name="mix_cols",
    )(*args)


def spans(sizes):
    lo = 0
    for size in sizes:
        yield lo, size
        lo += size


def solution(mesh):
    n_group, n_side = mesh.shape["expert"], mesh.shape["data"]
    tok_spec = P(("rep", "expert", "data"), None)
    wide_spec = P("expert", "data", None)
    down_spec = P("expert", None, "data")
    swap = [(s, 1 - s) for s in range(n_side)]

    def whole_step(x_loc, idx_loc, gate_loc, wg_loc, wu_loc, wd_loc):
        tok_rows, _ = x_loc.shape
        top_k = idx_loc.shape[1]
        n_local, half, ffn = wg_loc.shape
        n_exp = n_local * n_group
        capacity = capacity_rows(tok_rows, top_k, n_exp)
        side = lax.axis_index("data")
        place = lax.axis_index("expert")
        locals_ = range(n_local)
        groups = jnp.arange(n_group, dtype=I32)

        ids = ((idx_loc // n_local + n_group - place) % n_group * n_local + idx_loc % n_local).T
        experts = jnp.arange(n_exp, dtype=I32)[:, None]
        chosen = functools.reduce(jnp.logical_or, [ids[j][None, :] == experts for j in range(top_k)])
        chosen_i = chosen.astype(I32)
        running = jnp.cumsum(chosen_i, axis=1)
        before = running - chosen_i
        slot_te = jnp.where(chosen & (before < capacity), before, -1)
        counts = jnp.minimum(running[:, -1], capacity)
        first = jnp.minimum(before, capacity)
        first_blk = jnp.concatenate([first[:, ::TOK_BLOCK], counts[:, None]], axis=1).reshape(-1)
        first_mix = first[:, ::MIX_TILE]

        table = lax.all_gather(counts, "expert")
        meta = []
        for l in locals_:
            mine = jnp.sum(jnp.where(((place - groups) % n_group)[:, None, None] == groups[None, :, None], table.reshape(n_group, n_group, n_local)[None, :, :, l] * (groups[:, None, None] == groups[None, None, :]), 0), axis=(1, 2))
            ends = jnp.cumsum((mine + TILE - 1) // TILE)
            meta.append(jnp.concatenate([side[None], jnp.zeros((1,), I32), ends]).astype(I32))

        reach = REACH // ALIGN
        start = first_mix // ALIGN
        stop = jnp.concatenate([first_mix[:, 1:], counts[:, None]], axis=1)
        size = jnp.where(stop > first_mix, (stop + ALIGN - 1) // ALIGN - start, 0)
        lead = jnp.cumsum(size, axis=0) - size
        at = slot_te + jnp.repeat((lead - start) * ALIGN, MIX_TILE, axis=1)
        at = jnp.where(slot_te < 0, -1, at)
        pos = jnp.stack([jnp.sum(jnp.where(ids[j][None, :] == experts, at, 0), axis=0) for j in range(top_k)], axis=1)
        pairs = jnp.concatenate([pos.astype(F32), gate_loc], axis=1)
        seat = jnp.arange(reach, dtype=I32)[None, None, :]
        taken = (seat >= lead[:, :, None]) & (seat < (lead + size)[:, :, None])

        def chunk_table(array):
            source = array[:, :, None] * (capacity // ALIGN) + (start - lead)[:, :, None] + seat
            return (jnp.sum(jnp.where(taken, source, 0), axis=0) * ALIGN).reshape(-1)

        chunks = chunk_table(experts)

        done = []

        def in_turn(kernel, small, *args, follows=True):
            if done and follows:
                small = after(small, done[-1]) if done[-1].ndim else small + done[-1]
            out = kernel(small, *args)
            done.append(out[0] if isinstance(out, (list, tuple)) else out)
            return out

        wide_spans = list(spans(WIDE_CHUNKS))
        parts = [[w[0, :, : wide_spans[0][1]] for w in (wg_loc, wu_loc)]]
        later = after((wg_loc, wu_loc), parts[0])
        parts += [jnp.stack([w[l, :, lo : lo + n] for w in later]) for l in locals_ for lo, n in wide_spans if l or lo]
        far = []

        def cross():
            if len(far) == len(parts):
                return
            piece = parts[len(far)]
            if len(far) >= 2:
                piece = after(piece, far[-2])
            far.append(lax.ppermute(piece, "data", swap))

        def exchange(blocks, step):
            out = [blocks[0]]
            for d in range(1, n_group):
                out.append(lax.ppermute(blocks[d], "expert", [(s, (s + step * d) % n_group) for s in range(n_group)]))
            return out

        def mix(y_loc, chunks, *sets):
            col = jnp.stack([col for col, _, _ in sets]).astype(I32)
            back = [(pair[l][0][d], pair[l][1]) for _, _, pair in sets for d in range(n_group) for l in locals_]
            out = in_turn(mix_cols, col, y_loc, x_loc, pairs, chunks, tuple(width for _, width, _ in sets), back)
            done[-1] = out[1][0]
            return out[0]

        cross()
        cross()
        first_blk = after(first_blk, meta)
        rows = [exchange(in_turn(pack_rows, first_blk, x_loc, slot_te, n_exp, n_local, 0, capacity), 1)]
        cross()
        packed = in_turn(pack_rows, first_blk, x_loc, slot_te, n_exp, n_local, 1, capacity)
        cross()
        rows.append(exchange([after(block, rows[0]) for block in packed], 1))

        n_wide = len(wide_spans)
        hidden, own = [], []
        for l in locals_:
            hidden.append(None)
            for k, (lo, n) in enumerate(wide_spans):
                if k >= 2 or (l and k):
                    cross()
                hidden[l] = in_turn(wide_part, meta[l], hidden[l], rows[l], wg_loc, wu_loc, far[l * n_wide + k], l, lo, n, follows=k == 0)
                if not (l or k):
                    at_group = (groups[:, None, None] + groups[None, :, None]) % n_group == groups[None, None, :]
                    held = table.reshape(n_group, n_group, 1, n_local)
                    totals = after(jnp.sum(jnp.where(at_group[..., None], held, 0), axis=(0, 1)), done[-1])
                    totals += lax.ppermute(totals, "data", swap)
            if l == 0:
                cross()
                flips = (totals[:, 1] > totals[:, 0]).astype(I32)
                flip = jnp.sum(jnp.where(groups == place, flips, 0))
                parts += [lax.dynamic_slice(wd_loc, ((r + flip) % n_local, 0, lo), (1, ffn, n))[0] for r, lo, n in DOWN_PIECES]
            own.append(exchange(in_turn(down_part, meta[l], [hidden[l]], wd_loc, n_group, l, follows=False), -1))

        role_meta = []
        for r in locals_:
            picked = jnp.where(flip == 1, meta[(r + 1) % n_local], meta[r])
            role_meta.append(jnp.concatenate([((r + flip) % n_local)[None], picked[1:]]))
        d_flips = jnp.sum(jnp.where(((place + groups) % n_group)[:, None] == groups[None, :], flips[None, :], 0), axis=1)
        roles = (jnp.arange(n_local, dtype=I32)[None, :] + d_flips[:, None]) % n_local
        far_chunks = chunk_table((groups[:, None] * n_local + roles).reshape(n_exp, 1))

        def far_piece(i):
            cross()
            r = DOWN_PIECES[i][0]
            return exchange(in_turn(down_part, role_meta[r], hidden, far[n_local * n_wide + i], n_group), -1)

        far_col = (1 - side) * half
        ret = [far_piece(0), far_piece(1)]
        y_loc = mix(None, chunks, (side * half, half, [(own[l], 0) for l in locals_]))
        ret += [far_piece(2), far_piece(3)]
        y_loc = mix(y_loc, far_chunks, (far_col, 512, [(ret[0], 0), (ret[1], 0)]))
        ret.append(far_piece(4))
        y_loc = mix(y_loc, far_chunks, (far_col + 512, 256, [(ret[2], 0), (ret[3], 0)]))
        ret += [far_piece(5), far_piece(6)]
        y_loc = mix(y_loc, far_chunks, (far_col + 768, 128, [(ret[4], 0), (ret[5], 0)]))
        return mix(y_loc, far_chunks, (far_col + 896, 128, [(ret[4], 1), (ret[6], 0)]))

    in_specs = (tok_spec, tok_spec, tok_spec, wide_spec, wide_spec, down_spec)
    return jax.shard_map(whole_step, mesh=mesh, in_specs=in_specs, out_specs=tok_spec, check_vma=False)
```
